128 devices in a mesh: gz: 2 (over x_lo), gx: 2 (over core), gy: 32 (over z, y, x_hi).
Axes of the slice: x: 4 (x_hi: 2, x_lo: 2; x = x_hi * 2 + x_lo), y: 4, z: 4, core: 2. Of those that a mesh axis runs over, the one named last changes fastest.
Arguments:
- initial_field: float32 [128, 16, 4096], P('gz', 'gx', 'gy'), may hold values from -36 to 36
- plane_coupling: float32 [128, 16, 4096], P('gz', 'gx', 'gy'), may hold values from 0.06 to 0.24
- line_coupling: float32 [128, 16, 4096], P('gz', 'gx', 'gy'), may hold values from 1000 to 8000
- source: float32 [128, 16, 4096], P('gz', 'gx', 'gy'), may hold values from -4 to 4, as said below
- shift_table: float32 [8], replicated, may hold values from 0.5 to 1
- shift_index: int32 [4], replicated, may hold values from 0 to 7
Outputs:
- heated: float32 [128, 16, 4096], P('gz', 'gx', 'gy')
The draws below stay inside these ranges and needn't reach their ends.
Inputs may be any that keep to these rules, and one draw needn't show every extreme that they name: `shift_index`: one table row for each half-step. A heat source.
All inputs are finite; a program needn't handle non-finite values.
Results may differ from the reference program's by a relative error of at most 0.0003.
Values sent between devices are 32-bit elements; how exact they have to be, the bound alone decides.
A program may use at most 64 MiB of HBM per device.

```python
import math
import jax
import jax.numpy as jnp
from jax import lax

SHIFTS = 8
HALF = 4
NX = 16
NY = 4096
NZ = 128


def draw_source(key, part):
    values = jnp.clip(jax.random.normal(key, (NZ, NX, NY), jnp.float32), -4.0, 4.0)
    return values


def place_ends(entries, rng, least, top_value):
    dims = entries.shape
    place = [jax.random.randint(jax.random.fold_in(rng, axis), (), 0, dims[axis]) for axis in range(len(dims))]
    entries = entries.at[tuple(place)].set(least)
    longest = dims.index(max(dims))
    place[longest] = (place[longest] + 1) % dims[longest]
    return entries.at[tuple(place)].set(top_value)


def block_scale(stream_key, dims, shards, low, top_value):
    level = 1.0
    for axis_at, blocks in shards:
        draws = jax.random.uniform(jax.random.fold_in(jax.random.fold_in(stream_key, 6), axis_at), (blocks,), jnp.float32, low / len(shards), top_value / len(shards))
        level = level * jnp.repeat(jnp.exp(draws), dims[axis_at] // blocks).reshape((-1,) + (1,) * (len(dims) - 1 - axis_at))
    return level


def centred(stream_key, dims, scale, most, shards=(), kind=jnp.bfloat16):
    loudness = block_scale(stream_key, dims, shards, -0.22, 0.18) if shards else 1.0
    array = jax.random.normal(stream_key, dims, jnp.float32) * scale * loudness
    return jnp.minimum(jnp.maximum(array, -most), most).astype(kind)


def setup_inputs(seed: int = 0) -> dict:
    seeds = jax.random.split(jax.random.key(seed), 7)
    initial_field = centred(seeds[0], (NZ, NX, NY), 6.0, 36.0, ((0, 2), (1, 2), (2, 32)), jnp.float32)
    plane_coupling = jnp.clip(jnp.exp(math.log(0.24) - 1.3862944 * jax.random.uniform(seeds[1], (NZ, NX, NY), jnp.float32) ** block_scale(seeds[1], (NZ, NX, NY), ((0, 2), (1, 2), (2, 32)), -0.2, 0.2)), 0.06, 0.24)
    line_coupling = jnp.clip(jnp.exp(math.log(8000.0) - 2.0794415 * jax.random.uniform(seeds[2], (NZ, NX, NY), jnp.float32) ** block_scale(seeds[2], (NZ, NX, NY), ((0, 2), (1, 2), (2, 32)), -0.2, 0.2)), 1000.0, 8000.0)
    source = draw_source(jax.random.fold_in(seeds[6], 71), 0)
    shift_table = jnp.clip(jax.random.uniform(seeds[4], (SHIFTS,), jnp.float32, 0.5, 1.0), 0.5, 1.0)
    shift_index = place_ends(jax.random.randint(seeds[5], (HALF,), 0, SHIFTS), jax.random.fold_in(seeds[5], 1), 0, SHIFTS - 1).astype(jnp.int32)
    return {"initial_field": initial_field, "plane_coupling": plane_coupling, "line_coupling": line_coupling, "source": source, "shift_table": shift_table, "shift_index": shift_index}


def lookup(shift_table, table_row):
    table_slots = jnp.arange(shift_table.shape[0], dtype=jnp.int32)
    return jnp.sum(jnp.where(table_slots == table_row, shift_table, jnp.zeros_like(shift_table)))


def plane_apply(current, coupling):
    padded = jnp.pad(current, ((0, 0), (1, 1), (1, 1)))
    beside_all = padded[:, 2:, 1:-1] + padded[:, :-2, 1:-1] + padded[:, 1:-1, 2:] + padded[:, 1:-1, :-2]
    return coupling * (beside_all - 4.0 * current)


def line_solve(explicit, line_coupling, shift_value):
    scaled = shift_value * line_coupling
    center = 1.0 + 2.0 * scaled

    def forward(previous, inputs):
        before_c, before_d = previous
        coupling, middle, right_side = inputs
        pivot_value = middle + coupling * before_c
        next_c = -coupling / pivot_value
        next_d = (right_side + coupling * before_d) / pivot_value
        return (next_c, next_d), (next_c, next_d)

    zero_plane = jnp.zeros_like(explicit[0])
    final_state, factors = lax.scan(forward, (zero_plane, zero_plane), (scaled, center, explicit))

    def backward(later_value, inputs):
        ratio, offset = inputs
        own_value = offset - ratio * later_value
        return own_value, own_value

    final_value, solved = lax.scan(backward, zero_plane, factors, reverse=True)
    return solved


def reference(initial_field, plane_coupling, line_coupling, source, shift_table, shift_index):
    current = initial_field
    for half_step in range(HALF):
        shift_value = lookup(shift_table, shift_index[half_step])
        explicit = current + shift_value * (plane_apply(current, plane_coupling) + source)
        current = line_solve(explicit, line_coupling, shift_value)
    return current
```

```python
import functools
import jax
import jax.numpy as jnp
from jax import lax
from jax.experimental import pallas as pl
from jax.experimental.pallas import tpu as pltpu
from jax.sharding import PartitionSpec as P

HALF = 4
ROWS = 8
LANES = 128
UNROLL = 4
FIELD, PLANE, LINE, SOURCE = range(4)
MESH = pl.DeviceIdType.MESH


def kernel(
    columns,
    field_hbm, plane_hbm, line_hbm, source_hbm, table_hbm, index_hbm,
    out_hbm,
    table, index, block, theta, weight, inverse, state, packed, halo,
    pivots, pivots_in, mixed, planes, planes_in, result,
    local_sem, scalar_sem, out_sem,
    swap_send, swap_recv, far_send, far_recv, pass_send, pass_recv,
    pivot_send, pivot_recv, plane_send, plane_recv,
):
    layers = field_hbm.shape[0]
    gz, gx, gy = lax.axis_index("gz"), lax.axis_index("gx"), lax.axis_index("gy")
    has_left, has_right = gy > 0, gy < columns - 1
    lane = lax.broadcasted_iota(jnp.int32, (ROWS, LANES), 1)
    row = lax.broadcasted_iota(jnp.int32, (ROWS, LANES), 0)
    zero = jnp.zeros((ROWS, LANES), jnp.float32)
    one = jnp.ones((ROWS, LANES), jnp.float32)

    def layer(k):
        return gz * (layers - 1) + (1 - 2 * gz) * k

    loads = [
        pltpu.make_async_copy(source, block.at[a, gx], local_sem.at[a])
        for a, source in enumerate((field_hbm, plane_hbm, line_hbm, source_hbm))
    ]
    scalars = [
        pltpu.make_async_copy(table_hbm, table, scalar_sem.at[0]),
        pltpu.make_async_copy(index_hbm, index, scalar_sem.at[1]),
    ]
    for copy in scalars + loads:
        copy.start()

    barrier = pltpu.get_barrier_semaphore()
    pl.semaphore_signal(barrier, inc=1, device_id={"gx": 1 - gx}, device_id_type=MESH)
    pl.semaphore_signal(barrier, inc=1, device_id={"gz": 1 - gz}, device_id_type=MESH)

    @pl.when(has_left)
    def _():
        pl.semaphore_signal(barrier, inc=1, device_id={"gy": gy - 1}, device_id_type=MESH)

    @pl.when(has_right)
    def _():
        pl.semaphore_signal(barrier, inc=1, device_id={"gy": gy + 1}, device_id_type=MESH)

    for copy in scalars:
        copy.wait()
    shifts = [jnp.full((ROWS, LANES), table[index[h]], jnp.float32) for h in range(HALF)]
    inverses = [1.0 / s for s in shifts]

    for copy in loads:
        copy.wait()

    slots = LANES // 8
    groups = layers // (2 * slots)

    def pack(j, _):
        for a in range(4):
            left, right = zero, zero
            for b in range(2):
                for i in range(slots):
                    p = 8 * i + 4 * b
                    moved = block[a, gx, j * 2 * slots + b * slots + i]
                    if p:
                        moved = pltpu.roll(moved, p, 1)
                    at = lane // 4
                    right = jnp.where(at == p // 4, moved, right)
                    left = jnp.where(at == (p // 4 - 1) % 32, moved, left)
            packed[0, a * groups + j] = left
            packed[1, a * groups + j] = right
        return 0

    lax.fori_loop(0, groups, pack, 0)

    for side, missing in ((0, jnp.logical_not(has_left)), (1, jnp.logical_not(has_right))):
        @pl.when(missing)
        def _(side=side):
            for r in range(2):
                for a in range(4):
                    for j in range(groups):
                        halo[side, r, a * groups + j] = one * 1000.0 if a == LINE else zero

    def factor(q):
        def steps(t, carry):
            carry = list(carry)
            for s in range(UNROLL):
                k = layer(t * UNROLL + s)
                line = 1.0 / block[LINE, q, k]
                for h in range(HALF):
                    th, de = carry[2 * h], carry[2 * h + 1]
                    ratio = line * inverses[h]
                    w = ratio * th
                    de = de + w
                    new = th + de
                    theta[h, q, k] = th
                    weight[h, q, k] = w
                    inverse[h, q, k] = 1.0 / (new * th)
                    carry[2 * h], carry[2 * h + 1] = new, de
            return tuple(carry)

        end = lax.fori_loop(0, layers // UNROLL, steps, (one,) * (2 * HALF))
        for h in range(HALF):
            pivots[q, h, 0] = end[2 * h]
            pivots[q, h, 1] = end[2 * h + 1]

    factor(gx)

    signals = 2 + has_left.astype(jnp.int32) + has_right.astype(jnp.int32)
    pl.semaphore_wait(barrier, signals)

    def far(side):
        return pltpu.make_async_remote_copy(
            src_ref=packed.at[side],
            dst_ref=halo.at[side, gx],
            send_sem=far_send.at[side],
            recv_sem=far_recv.at[side],
            device_id={"gy": gy + 1 - 2 * side},
            device_id_type=MESH,
        )

    @pl.when(has_right)
    def _():
        far(0).start()

    @pl.when(has_left)
    def _():
        far(1).start()

    swaps = [
        pltpu.make_async_remote_copy(
            src_ref=block.at[a, gx],
            dst_ref=block.at[a, gx],
            send_sem=swap_send.at[a],
            recv_sem=swap_recv.at[a],
            device_id={"gx": 1 - gx},
            device_id_type=MESH,
        )
        for a in (LINE, FIELD, PLANE, SOURCE)
    ]
    for copy in swaps:
        copy.start()
    for copy in swaps:
        copy.wait_recv()
    factor(1 - gx)

    def pivot_copy(e):
        return pltpu.make_async_remote_copy(
            src_ref=pivots.at[pl.ds(2 * e, 2)],
            dst_ref=pivots_in.at[pl.ds(2 * e, 2)],
            send_sem=pivot_send.at[e],
            recv_sem=pivot_recv.at[e],
            device_id={"gz": 1 - gz},
            device_id_type=MESH,
        )

    pivot_copy(0).start()

    def passed(side):
        return pltpu.make_async_remote_copy(
            src_ref=halo.at[side, gx],
            dst_ref=halo.at[side, gx],
            send_sem=pass_send.at[side],
            recv_sem=pass_recv.at[side],
            device_id={"gx": 1 - gx},
            device_id_type=MESH,
        )

    for side, there in ((0, has_left), (1, has_right)):
        @pl.when(there)
        def _(side=side):
            far(side).wait_recv()
            passed(side).start()

    for side, there in ((0, has_left), (1, has_right)):
        @pl.when(there)
        def _(side=side):
            passed(side).wait_recv()

    odd = lax.rem(lane // 4, 2) == 1

    def unpack(j, _):
        for a in range(4):
            for r in range(2):
                left = halo[0, r, a * groups + j]
                right = halo[1, r, a * groups + j]
                for b in range(2):
                    both = jnp.where(odd, right, left) if b else jnp.where(odd, left, right)
                    for i in range(slots):
                        p = 8 * i + 4 * b
                        block[a, 2 + r, j * 2 * slots + b * slots + i] = (
                            pltpu.roll(both, LANES - p, 1) if p else both
                        )
        return 0

    lax.fori_loop(0, groups, unpack, 0)
    factor(2)
    factor(3)
    pivot_copy(1).start()
    pivot_copy(0).wait_recv()
    pivot_copy(1).wait_recv()
    for q in range(4):
        for h in range(HALF):
            last, step = pivots[q, h, 0], pivots[q, h, 1]
            other_last, other_step = pivots_in[q, h, 0], pivots_in[q, h, 1]
            before = last - step
            share = 1.0 / (before * other_step + step * other_last)
            mixed[q, h, 0] = other_last * share / before
            mixed[q, h, 1] = share

    first, final = lane == 0, lane == LANES - 1
    top, bottom = row == 0, row == ROWS - 1

    def spread(u):
        ups = [pltpu.roll(x, 1, 0) for x in u]
        downs = [pltpu.roll(x, ROWS - 1, 0) for x in u]
        lefts = [pltpu.roll(x, 1, 1) for x in u]
        rights = [pltpu.roll(x, LANES - 1, 1) for x in u]
        sums = []
        for q in range(4):
            r, twin = q % 2, (q + 2) % 4
            up = jnp.where(top, ups[q - 1] if r else zero, ups[q])
            down = jnp.where(bottom, zero if r else downs[q + 1], downs[q])
            left = jnp.where(first, lefts[twin], lefts[q])
            right = jnp.where(final, rights[twin], rights[q])
            sums.append((up + down) + (left + right))
        return sums

    def plane_copy(h):
        return pltpu.make_async_remote_copy(
            src_ref=planes.at[h],
            dst_ref=planes_in.at[h],
            send_sem=plane_send.at[h],
            recv_sem=plane_recv.at[h],
            device_id={"gz": 1 - gz},
            device_id_type=MESH,
        )

    ends = [zero] * 4
    for h in range(HALF):
        shift = shifts[h]

        def forward(t, total, h=h, shift=shift, ends=ends):
            total = list(total)
            for s in range(UNROLL):
                k = layer(t * UNROLL + s)
                if h == 0:
                    u = [block[FIELD, q, k] for q in range(4)]
                else:
                    u = [theta[h - 1, q, k] * (state[q, k] + ends[q]) for q in range(4)]
                beside = spread(u)
                for q in range(4):
                    flux = block[PLANE, q, k] * (beside[q] - 4.0 * u[q]) + block[SOURCE, q, k]
                    explicit = u[q] + shift * flux
                    total[q] = total[q] + weight[h, q, k] * explicit
                    state[q, k] = inverse[h, q, k] * total[q]
            return tuple(total)

        total = lax.fori_loop(0, layers // UNROLL, forward, (zero,) * 4)
        for q in range(4):
            planes[h, q] = total[q]
        plane_copy(h).start()

        def backward(t, later, h=h):
            later = list(later)
            for s in range(UNROLL):
                k = layer(layers - 1 - (t * UNROLL + s))
                for q in range(4):
                    here = state[q, k]
                    if s == 0:
                        here = jnp.where(t == 0, zero, here)
                    later[q] = later[q] + here
                    state[q, k] = later[q]
            return tuple(later)

        lax.fori_loop(0, layers // UNROLL, backward, (zero,) * 4)
        plane_copy(h).wait_recv()
        ends = [
            mixed[q, h, 0] * planes[h, q] + mixed[q, h, 1] * planes_in[h, q] for q in range(4)
        ]

    own_end = jnp.where(gx == 0, ends[0], ends[1])

    def finish(t, _):
        for s in range(UNROLL):
            k = t * UNROLL + s
            result[k] = theta[HALF - 1, gx, k] * (state[gx, k] + own_end)
        return 0

    lax.fori_loop(0, layers // UNROLL, finish, 0)
    store = pltpu.make_async_copy(result, out_hbm, out_sem)
    store.start()

    for copy in swaps:
        copy.wait_send()
    for side, there in ((0, has_left), (1, has_right)):
        @pl.when(there)
        def _(side=side):
            passed(side).wait_send()

    @pl.when(has_right)
    def _():
        far(0).wait_send()

    @pl.when(has_left)
    def _():
        far(1).wait_send()

    for e in range(2):
        pivot_copy(e).wait_send()
    for h in range(HALF):
        plane_copy(h).wait_send()
    store.wait()


def on_device(columns, field, plane, line, source, table, index):
    layers = field.shape[0]
    tile = (ROWS, LANES)
    f32 = jnp.float32
    groups = layers // 32
    dma = pltpu.SemaphoreType.DMA
    return pl.pallas_call(
        functools.partial(kernel, columns),
        out_shape=jax.ShapeDtypeStruct(field.shape, f32),
        in_specs=[pl.BlockSpec(memory_space=pltpu.HBM)] * 6,
        out_specs=pl.BlockSpec(memory_space=pltpu.HBM),
        scratch_shapes=[
            pltpu.SMEM(table.shape, f32),
            pltpu.SMEM(index.shape, jnp.int32),
            pltpu.VMEM((4, 4, layers, *tile), f32),
            pltpu.VMEM((HALF, 4, layers, *tile), f32),
            pltpu.VMEM((HALF, 4, layers, *tile), f32),
            pltpu.VMEM((HALF, 4, layers, *tile), f32),
            pltpu.VMEM((4, layers, *tile), f32),
            pltpu.VMEM((2, 4 * groups, *tile), f32),
            pltpu.VMEM((2, 2, 4 * groups, *tile), f32),
            pltpu.VMEM((4, HALF, 2, *tile), f32),
            pltpu.VMEM((4, HALF, 2, *tile), f32),
            pltpu.VMEM((4, HALF, 2, *tile), f32),
            pltpu.VMEM((HALF, 4, *tile), f32),
            pltpu.VMEM((HALF, 4, *tile), f32),
            pltpu.VMEM((layers, *tile), f32),
            dma((4,)), dma((2,)), dma,
            dma((4,)), dma((4,)), dma((2,)), dma((2,)), dma((2,)), dma((2,)),
            dma((2,)), dma((2,)), dma((HALF,)), dma((HALF,)),
        ],
        compiler_params=pltpu.CompilerParams(
            collective_id=0, has_side_effects=True, vmem_limit_bytes=67043328
        ),
    )(field, plane, line, source, table, index)


def solution(mesh):
    spec = P("gz", "gx", "gy")
    return jax.shard_map(
        functools.partial(on_device, mesh.shape["gy"]),
        mesh=mesh,
        in_specs=(spec, spec, spec, spec, P(), P()),
        out_specs=spec,
        check_vma=False,
    )
```

```python
import functools
import jax
import jax.numpy as jnp
from jax import lax
from jax.experimental import pallas as pl
from jax.experimental.pallas import tpu as pltpu
from jax.sharding import PartitionSpec as P

HALF = 4
ROWS = 8
LANES = 128
UNROLL = 16
FIELD, PLANE, LINE, SOURCE = range(4)
MESH = pl.DeviceIdType.MESH


def kernel(
    columns,
    field_hbm, plane_hbm, line_hbm, source_hbm, table_hbm, index_hbm,
    out_hbm,
    table, index, raw, block, theta, weight, inverse, state, packed, halo,
    pivots, pivots_in, edge, edge_in, mixed, planes, planes_in, result,
    local_sem, scalar_sem, out_sem,
    swap_send, swap_recv, far_send, far_recv, pass_send, pass_recv,
    pivot_send, pivot_recv, edge_send, edge_recv, plane_send, plane_recv,
):
    layers = field_hbm.shape[0]
    gz, gx, gy = lax.axis_index("gz"), lax.axis_index("gx"), lax.axis_index("gy")
    has_left, has_right = gy > 0, gy < columns - 1
    lane = lax.broadcasted_iota(jnp.int32, (ROWS, LANES), 1)
    row = lax.broadcasted_iota(jnp.int32, (ROWS, LANES), 0)
    zero = jnp.zeros((ROWS, LANES), jnp.float32)
    one = jnp.ones((ROWS, LANES), jnp.float32)

    def layer(k):
        return gz * (layers - 1) + (1 - 2 * gz) * k

    loads = [
        pltpu.make_async_copy(source, raw.at[a], local_sem.at[a])
        for a, source in enumerate((field_hbm, plane_hbm, line_hbm, source_hbm))
    ]
    scalars = [
        pltpu.make_async_copy(table_hbm, table, scalar_sem.at[0]),
        pltpu.make_async_copy(index_hbm, index, scalar_sem.at[1]),
    ]
    for copy in scalars + loads:
        copy.start()

    barrier = pltpu.get_barrier_semaphore()
    pl.semaphore_signal(barrier, inc=1, device_id={"gx": 1 - gx}, device_id_type=MESH)
    pl.semaphore_signal(barrier, inc=1, device_id={"gz": 1 - gz}, device_id_type=MESH)
    pl.semaphore_signal(
        barrier, inc=1, device_id={"gz": 1 - gz, "gx": 1 - gx}, device_id_type=MESH
    )

    @pl.when(has_left)
    def _():
        pl.semaphore_signal(barrier, inc=1, device_id={"gy": gy - 1}, device_id_type=MESH)

    @pl.when(has_right)
    def _():
        pl.semaphore_signal(barrier, inc=1, device_id={"gy": gy + 1}, device_id_type=MESH)

    for copy in scalars:
        copy.wait()
    shifts = [jnp.full((ROWS, LANES), table[index[h]], jnp.float32) for h in range(HALF)]
    inverses = [1.0 / s for s in shifts]

    for copy in loads:
        copy.wait()

    def arrange(t, _):
        for s in range(UNROLL):
            k = t * UNROLL + s
            at = layer(k)
            for a in range(4):
                block[a, gx, k] = raw[a, at]
        return 0

    lax.fori_loop(0, layers // UNROLL, arrange, 0)

    slots = LANES // 8
    groups = layers // (2 * slots)

    def pack(j, _):
        for a in range(4):
            left, right = zero, zero
            for b in range(2):
                for i in range(slots):
                    p = 8 * i + 4 * b
                    moved = block[a, gx, j * 2 * slots + b * slots + i]
                    if p:
                        moved = pltpu.roll(moved, p, 1)
                    at = lane // 4
                    right = jnp.where(at == p // 4, moved, right)
                    left = jnp.where(at == (p // 4 - 1) % 32, moved, left)
            packed[0, a * groups + j] = left
            packed[1, a * groups + j] = right
        return 0

    lax.fori_loop(0, groups, pack, 0)

    for side, missing in ((0, jnp.logical_not(has_left)), (1, jnp.logical_not(has_right))):
        @pl.when(missing)
        def _(side=side):
            for r in range(2):
                for a in range(4):
                    for j in range(groups):
                        halo[side, r, a * groups + j] = one * 1000.0 if a == LINE else zero

    def factor(q):
        def steps(t, carry):
            carry = list(carry)
            for s in range(UNROLL):
                k = t * UNROLL + s
                line = 1.0 / block[LINE, q, k]
                for h in range(HALF):
                    th, de = carry[2 * h], carry[2 * h + 1]
                    ratio = line * inverses[h]
                    w = ratio * th
                    de = de + w
                    new = th + de
                    theta[h, q, k] = th
                    weight[h, q, k] = w
                    inverse[h, q, k] = 1.0 / (new * th)
                    carry[2 * h], carry[2 * h + 1] = new, de
            return tuple(carry)

        end = lax.fori_loop(0, layers // UNROLL, steps, (one,) * (2 * HALF))
        for h in range(HALF):
            pivots[q, h, 0] = end[2 * h]
            pivots[q, h, 1] = end[2 * h + 1]

    factor(gx)

    signals = 3 + has_left.astype(jnp.int32) + has_right.astype(jnp.int32)
    pl.semaphore_wait(barrier, signals)

    def far(side):
        return pltpu.make_async_remote_copy(
            src_ref=packed.at[side],
            dst_ref=halo.at[side, gx],
            send_sem=far_send.at[side],
            recv_sem=far_recv.at[side],
            device_id={"gy": gy + 1 - 2 * side},
            device_id_type=MESH,
        )

    @pl.when(has_right)
    def _():
        far(0).start()

    @pl.when(has_left)
    def _():
        far(1).start()

    def pivot_copy(e):
        return pltpu.make_async_remote_copy(
            src_ref=pivots.at[gx],
            dst_ref=pivots_in.at[gx],
            send_sem=pivot_send.at[e],
            recv_sem=pivot_recv.at[e],
            device_id={"gz": 1 - gz, "gx": lax.rem(gx + e, 2)},
            device_id_type=MESH,
        )

    def pivot_arrival(e):
        return pltpu.make_async_remote_copy(
            src_ref=pivots.at[gx],
            dst_ref=pivots_in.at[lax.rem(gx + e, 2)],
            send_sem=pivot_send.at[e],
            recv_sem=pivot_recv.at[e],
            device_id={"gz": 1 - gz, "gx": lax.rem(gx + e, 2)},
            device_id_type=MESH,
        )

    for e in range(2):
        pivot_copy(e).start()

    swaps = [
        pltpu.make_async_remote_copy(
            src_ref=block.at[a, gx],
            dst_ref=block.at[a, gx],
            send_sem=swap_send.at[a],
            recv_sem=swap_recv.at[a],
            device_id={"gx": 1 - gx},
            device_id_type=MESH,
        )
        for a in (LINE, FIELD, PLANE, SOURCE)
    ]
    for copy in swaps:
        copy.start()
    swaps[0].wait_recv()
    factor(1 - gx)
    for copy in swaps[1:]:
        copy.wait_recv()

    def passed(side):
        return pltpu.make_async_remote_copy(
            src_ref=halo.at[side, gx],
            dst_ref=halo.at[side, gx],
            send_sem=pass_send.at[side],
            recv_sem=pass_recv.at[side],
            device_id={"gx": 1 - gx},
            device_id_type=MESH,
        )

    for side, there in ((0, has_left), (1, has_right)):
        @pl.when(there)
        def _(side=side):
            far(side).wait_recv()
            passed(side).start()

    for side, there in ((0, has_left), (1, has_right)):
        @pl.when(there)
        def _(side=side):
            passed(side).wait_recv()

    odd = lax.rem(lane // 4, 2) == 1

    def unpack(j, _):
        for a in range(4):
            for r in range(2):
                left = halo[0, r, a * groups + j]
                right = halo[1, r, a * groups + j]
                for b in range(2):
                    both = jnp.where(odd, right, left) if b else jnp.where(odd, left, right)
                    for i in range(slots):
                        p = 8 * i + 4 * b
                        block[a, 2 + r, j * 2 * slots + b * slots + i] = (
                            pltpu.roll(both, LANES - p, 1) if p else both
                        )
        return 0

    lax.fori_loop(0, groups, unpack, 0)
    factor(2)
    factor(3)
    window = lax.rem(lane + 4, LANES) // 8

    def edge_copy():
        return pltpu.make_async_remote_copy(
            src_ref=edge,
            dst_ref=edge_in,
            send_sem=edge_send,
            recv_sem=edge_recv,
            device_id={"gz": 1 - gz},
            device_id_type=MESH,
        )

    slot = 0
    gathered = zero
    for q in (2, 3):
        for h in range(HALF):
            for c in range(2):
                moved = pivots[q, h, c]
                if slot:
                    moved = pltpu.roll(moved, 8 * slot, 1)
                gathered = jnp.where(window == slot, moved, gathered)
                slot += 1
    edge[...] = gathered
    edge_copy().start()

    def mix(q, h, other_last, other_step):
        last, step = pivots[q, h, 0], pivots[q, h, 1]
        before = last - step
        share = 1.0 / (before * other_step + step * other_last)
        ratio = other_last * share / before
        if q >= 2:
            share = jnp.where(window == 0, share, 0.0)
            ratio = jnp.where(window == 0, ratio, 0.0)
        mixed[q, h, 0] = ratio
        mixed[q, h, 1] = share

    for e in range(2):
        pivot_arrival(e).wait_recv()
    for q in range(2):
        for h in range(HALF):
            mix(q, h, pivots_in[q, h, 0], pivots_in[q, h, 1])

    first, final = lane == 0, lane == LANES - 1
    top, bottom = row == 0, row == ROWS - 1

    def spread(u):
        ups = [pltpu.roll(x, 1, 0) for x in u]
        downs = [pltpu.roll(x, ROWS - 1, 0) for x in u]
        lefts = [pltpu.roll(x, 1, 1) for x in u]
        rights = [pltpu.roll(x, LANES - 1, 1) for x in u]
        sums = []
        for q in range(4):
            r, twin = q % 2, (q + 2) % 4
            up = jnp.where(top, ups[q - 1] if r else zero, ups[q])
            down = jnp.where(bottom, zero if r else downs[q + 1], downs[q])
            left = jnp.where(first, lefts[twin], lefts[q])
            right = jnp.where(final, rights[twin], rights[q])
            sums.append((up + down) + (left + right))
        return sums

    def plane_copy(h):
        return pltpu.make_async_remote_copy(
            src_ref=planes.at[h],
            dst_ref=planes_in.at[h],
            send_sem=plane_send.at[h],
            recv_sem=plane_recv.at[h],
            device_id={"gz": 1 - gz},
            device_id_type=MESH,
        )

    ends = [zero] * 4
    for h in range(HALF):
        shift = shifts[h]

        def forward(t, total, h=h, shift=shift, ends=ends):
            total = list(total)
            for s in range(UNROLL):
                k = t * UNROLL + s
                if h == 0:
                    u = [block[FIELD, q, k] for q in range(4)]
                else:
                    u = [theta[h - 1, q, k] * (state[q, k] + ends[q]) for q in range(4)]
                beside = spread(u)
                for q in range(4):
                    flux = block[PLANE, q, k] * (beside[q] - 4.0 * u[q]) + block[SOURCE, q, k]
                    explicit = u[q] + shift * flux
                    total[q] = total[q] + weight[h, q, k] * explicit
                    state[q, k] = inverse[h, q, k] * total[q]
            return tuple(total)

        total = lax.fori_loop(0, layers // UNROLL, forward, (zero,) * 4)
        for q in range(2):
            planes[h, q] = total[q]
        planes[h, 2] = jnp.where(window == 0, total[2], pltpu.roll(total[3], LANES // 2, 1))
        plane_copy(h).start()

        def backward(t, later, h=h):
            later = list(later)
            for s in range(UNROLL):
                k = layers - 1 - (t * UNROLL + s)
                for q in range(4):
                    here = state[q, k]
                    if s == 0:
                        here = jnp.where(t == 0, zero, here)
                    later[q] = later[q] + here
                    state[q, k] = later[q]
            return tuple(later)

        lax.fori_loop(0, layers // UNROLL, backward, (zero,) * 4)
        if h == 0:
            edge_copy().wait_recv()
            arrived = edge_in[...]
            for q in (2, 3):
                for i in range(HALF):
                    slot = ((q - 2) * HALF + i) * 2
                    pair = [
                        pltpu.roll(arrived, (LANES - 8 * c) % LANES, 1) if c else arrived
                        for c in (slot, slot + 1)
                    ]
                    mix(q, i, jnp.where(window == 0, pair[0], 1.0), jnp.where(window == 0, pair[1], 1.0))
        plane_copy(h).wait_recv()
        there = [planes_in[h, q] for q in range(3)]
        there.append(pltpu.roll(there[2], LANES // 2, 1))
        ends = [mixed[q, h, 0] * total[q] + mixed[q, h, 1] * there[q] for q in range(4)]

    own_end = jnp.where(gx == 0, ends[0], ends[1])

    def finish(t, _):
        for s in range(UNROLL):
            k = t * UNROLL + s
            result[layer(k)] = theta[HALF - 1, gx, k] * (state[gx, k] + own_end)
        return 0

    lax.fori_loop(0, layers // UNROLL, finish, 0)
    store = pltpu.make_async_copy(result, out_hbm, out_sem)
    store.start()

    for copy in swaps:
        copy.wait_send()
    for side, there in ((0, has_left), (1, has_right)):
        @pl.when(there)
        def _(side=side):
            passed(side).wait_send()

    @pl.when(has_right)
    def _():
        far(0).wait_send()

    @pl.when(has_left)
    def _():
        far(1).wait_send()

    for e in range(2):
        pivot_copy(e).wait_send()
    edge_copy().wait_send()
    for h in range(HALF):
        plane_copy(h).wait_send()
    store.wait()


def on_device(columns, field, plane, line, source, table, index):
    layers = field.shape[0]
    tile = (ROWS, LANES)
    f32 = jnp.float32
    groups = layers // 32
    dma = pltpu.SemaphoreType.DMA
    return pl.pallas_call(
        functools.partial(kernel, columns),
        out_shape=jax.ShapeDtypeStruct(field.shape, f32),
        in_specs=[pl.BlockSpec(memory_space=pltpu.HBM)] * 6,
        out_specs=pl.BlockSpec(memory_space=pltpu.HBM),
        scratch_shapes=[
            pltpu.SMEM(table.shape, f32),
            pltpu.SMEM(index.shape, jnp.int32),
            pltpu.VMEM((4, layers, *tile), f32),
            pltpu.VMEM((4, 4, layers, *tile), f32),
            pltpu.VMEM((HALF, 4, layers, *tile), f32),
            pltpu.VMEM((HALF, 4, layers, *tile), f32),
            pltpu.VMEM((HALF, 4, layers, *tile), f32),
            pltpu.VMEM((4, layers, *tile), f32),
            pltpu.VMEM((2, 4 * groups, *tile), f32),
            pltpu.VMEM((2, 2, 4 * groups, *tile), f32),
            pltpu.VMEM((4, HALF, 2, *tile), f32),
            pltpu.VMEM((2, HALF, 2, *tile), f32),
            pltpu.VMEM(tile, f32),
            pltpu.VMEM(tile, f32),
            pltpu.VMEM((4, HALF, 2, *tile), f32),
            pltpu.VMEM((HALF, 3, *tile), f32),
            pltpu.VMEM((HALF, 3, *tile), f32),
            pltpu.VMEM((layers, *tile), f32),
            dma((4,)), dma((2,)), dma,
            dma((4,)), dma((4,)), dma((2,)), dma((2,)), dma((2,)), dma((2,)),
            dma((2,)), dma((2,)), dma, dma, dma((HALF,)), dma((HALF,)),
        ],
        compiler_params=pltpu.CompilerParams(
            collective_id=0, has_side_effects=True, vmem_limit_bytes=67043328
        ),
    )(field, plane, line, source, table, index)


def solution(mesh):
    spec = P("gz", "gx", "gy")
    return jax.shard_map(
        functools.partial(on_device, mesh.shape["gy"]),
        mesh=mesh,
        in_specs=(spec, spec, spec, spec, P(), P()),
        out_specs=spec,
        check_vma=False,
    )
```

```python
import functools
import jax
import jax.numpy as jnp
from jax import lax
from jax.experimental import pallas as pl
from jax.experimental.pallas import tpu as pltpu
from jax.sharding import PartitionSpec as P

HALF = 4
ROWS = 8
LANES = 128
UNROLL = 16
FIELD, PLANE, LINE, SOURCE = range(4)
MESH = pl.DeviceIdType.MESH


def kernel(
    columns,
    field_hbm, plane_hbm, line_hbm, source_hbm, table_hbm, index_hbm,
    out_hbm,
    table, index, raw, block, theta, weight, inverse, state, packed, halo, halo_beside,
    row_out, row_in, theta_out, theta_in,
    pivots, pivots_in, edge, edge_in, mixed, planes, planes_in, result,
    local_sem, scalar_sem, out_sem,
    far_send, far_recv, beside_send, beside_recv, row_send, row_recv, theta_send, theta_recv,
    pivot_send, pivot_recv, edge_send, edge_recv, plane_send, plane_recv,
):
    layers = field_hbm.shape[0]
    gz, gx, gy = lax.axis_index("gz"), lax.axis_index("gx"), lax.axis_index("gy")
    has_left, has_right = gy > 0, gy < columns - 1
    lane = lax.broadcasted_iota(jnp.int32, (ROWS, LANES), 1)
    row = lax.broadcasted_iota(jnp.int32, (ROWS, LANES), 0)
    zero = jnp.zeros((ROWS, LANES), jnp.float32)
    one = jnp.ones((ROWS, LANES), jnp.float32)
    upper = jnp.full((ROWS, LANES), gx, jnp.int32) == 0

    def layer(k):
        return gz * (layers - 1) + (1 - 2 * gz) * k

    peers = (
        {"gx": 1 - gx},
        {"gz": 1 - gz},
        {"gz": 1 - gz, "gx": 1 - gx},
    )

    def facing(tile):
        return jnp.where(upper, pltpu.roll(tile, 1, 0), tile)

    def beyond(tile):
        first = jnp.broadcast_to(tile[0:1], (ROWS, LANES))
        last = jnp.broadcast_to(tile[ROWS - 1 : ROWS], (ROWS, LANES))
        return jnp.where(upper, first, last)

    loads = [
        pltpu.make_async_copy(source, raw.at[a], local_sem.at[a])
        for a, source in enumerate((field_hbm, plane_hbm, line_hbm, source_hbm))
    ]
    scalars = [
        pltpu.make_async_copy(table_hbm, table, scalar_sem.at[0]),
        pltpu.make_async_copy(index_hbm, index, scalar_sem.at[1]),
    ]
    for copy in scalars + loads:
        copy.start()

    barrier = pltpu.get_barrier_semaphore()
    for peer in peers:
        pl.semaphore_signal(barrier, inc=1, device_id=peer, device_id_type=MESH)

    @pl.when(has_left)
    def _():
        pl.semaphore_signal(barrier, inc=1, device_id={"gy": gy - 1}, device_id_type=MESH)
        pl.semaphore_signal(
            barrier, inc=1, device_id={"gy": gy - 1, "gx": 1 - gx}, device_id_type=MESH
        )

    @pl.when(has_right)
    def _():
        pl.semaphore_signal(barrier, inc=1, device_id={"gy": gy + 1}, device_id_type=MESH)
        pl.semaphore_signal(
            barrier, inc=1, device_id={"gy": gy + 1, "gx": 1 - gx}, device_id_type=MESH
        )

    for copy in scalars:
        copy.wait()
    shifts = [jnp.full((ROWS, LANES), table[index[h]], jnp.float32) for h in range(HALF)]
    inverses = [1.0 / s for s in shifts]

    for copy in loads:
        copy.wait()

    def arrange(t, _):
        for s in range(UNROLL):
            k = t * UNROLL + s
            at = layer(k)
            for a in range(4):
                block[a, 0, k] = raw[a, at]
            row_out[0, 0, pl.ds(k, 1)] = facing(raw[FIELD, at])[0:1]
        return 0

    lax.fori_loop(0, layers // UNROLL, arrange, 0)

    slots = LANES // 8
    groups = layers // (2 * slots)

    def pack(j, _):
        for a in range(4):
            left, right = zero, zero
            for b in range(2):
                for i in range(slots):
                    p = 8 * i + 4 * b
                    moved = block[a, 0, j * 2 * slots + b * slots + i]
                    if p:
                        moved = pltpu.roll(moved, p, 1)
                    at = lane // 4
                    right = jnp.where(at == p // 4, moved, right)
                    left = jnp.where(at == (p // 4 - 1) % 32, moved, left)
            packed[0, a * groups + j] = left
            packed[1, a * groups + j] = right
        return 0

    lax.fori_loop(0, groups, pack, 0)

    for side, missing in ((0, jnp.logical_not(has_left)), (1, jnp.logical_not(has_right))):
        @pl.when(missing)
        def _(side=side):
            for a in range(4):
                for j in range(groups):
                    halo[side, a * groups + j] = one * 1000.0 if a == LINE else zero
            for j in range(groups):
                halo_beside[side, j] = zero

    def factor(q):
        def steps(t, carry):
            carry = list(carry)
            for s in range(UNROLL):
                k = t * UNROLL + s
                line = 1.0 / block[LINE, q, k]
                for h in range(HALF):
                    th, de = carry[2 * h], carry[2 * h + 1]
                    ratio = line * inverses[h]
                    w = ratio * th
                    de = de + w
                    new = th + de
                    theta[h, q, k] = th
                    weight[h, q, k] = w
                    inverse[h, q, k] = 1.0 / (new * th)
                    if h < HALF - 1:
                        theta_out[q, h, pl.ds(k, 1)] = facing(th)[0:1]
                    carry[2 * h], carry[2 * h + 1] = new, de
            return tuple(carry)

        end = lax.fori_loop(0, layers // UNROLL, steps, (one,) * (2 * HALF))
        for h in range(HALF):
            pivots[q, h, 0] = end[2 * h]
            pivots[q, h, 1] = end[2 * h + 1]

    factor(0)

    signals = 3 + 2 * has_left.astype(jnp.int32) + 2 * has_right.astype(jnp.int32)
    pl.semaphore_wait(barrier, signals)

    def far(side):
        return pltpu.make_async_remote_copy(
            src_ref=packed.at[side],
            dst_ref=halo.at[side],
            send_sem=far_send.at[side],
            recv_sem=far_recv.at[side],
            device_id={"gy": gy + 1 - 2 * side},
            device_id_type=MESH,
        )

    def far_beside(side):
        return pltpu.make_async_remote_copy(
            src_ref=packed.at[side, pl.ds(FIELD * groups, groups)],
            dst_ref=halo_beside.at[side],
            send_sem=beside_send.at[side],
            recv_sem=beside_recv.at[side],
            device_id={"gy": gy + 1 - 2 * side, "gx": 1 - gx},
            device_id_type=MESH,
        )

    for side, there in ((0, has_right), (1, has_left)):
        @pl.when(there)
        def _(side=side):
            far(side).start()
            far_beside(side).start()

    def to_peer(source, target, send, recv, e):
        return pltpu.make_async_remote_copy(
            src_ref=source,
            dst_ref=target,
            send_sem=send,
            recv_sem=recv,
            device_id=peers[e],
            device_id_type=MESH,
        )

    def pivot_copy(e):
        return to_peer(pivots.at[0], pivots_in.at[e], pivot_send.at[e], pivot_recv.at[e], e)

    def edge_copy(e):
        return to_peer(edge, edge_in.at[e], edge_send.at[e], edge_recv.at[e], e)

    def plane_copy(h, e):
        return to_peer(
            planes.at[h], planes_in.at[h, e], plane_send.at[h, e], plane_recv.at[h, e], e
        )

    def theta_copy(q):
        return to_peer(theta_out.at[q], theta_in.at[q], theta_send.at[q], theta_recv.at[q], 0)

    def row_copy(h):
        return to_peer(row_out.at[h], row_in.at[h], row_send.at[h], row_recv.at[h], 0)

    first_rows = to_peer(row_out.at[0, 0], row_in.at[0, 0], row_send.at[0], row_recv.at[0], 0)

    first_rows.start()
    for e in range(3):
        pivot_copy(e).start()
    theta_copy(0).start()

    for side, there in ((0, has_left), (1, has_right)):
        @pl.when(there)
        def _(side=side):
            far(side).wait_recv()
            far_beside(side).wait_recv()

    odd = lax.rem(lane // 4, 2) == 1

    def unpack(j, _):
        for a in range(4):
            left, right = halo[0, a * groups + j], halo[1, a * groups + j]
            for b in range(2):
                both = jnp.where(odd, right, left) if b else jnp.where(odd, left, right)
                for i in range(slots):
                    p = 8 * i + 4 * b
                    block[a, 1, j * 2 * slots + b * slots + i] = (
                        pltpu.roll(both, LANES - p, 1) if p else both
                    )
        left, right = halo_beside[0, j], halo_beside[1, j]
        for b in range(2):
            both = jnp.where(odd, right, left) if b else jnp.where(odd, left, right)
            both = jnp.where(upper, both, pltpu.roll(both, 1, 0))
            for i in range(slots):
                p = 8 * i + 4 * b
                moved = pltpu.roll(both, LANES - p, 1) if p else both
                row_in[0, 1, pl.ds(j * 2 * slots + b * slots + i, 1)] = moved[0:1]
        return 0

    lax.fori_loop(0, groups, unpack, 0)
    factor(1)
    theta_copy(1).start()
    window = lax.rem(lane + 4, LANES) // 8
    slot = 0
    gathered = zero
    for h in range(HALF):
        for c in range(2):
            moved = pivots[1, h, c]
            if slot:
                moved = pltpu.roll(moved, 8 * slot, 1)
            gathered = jnp.where(window == slot, moved, gathered)
            slot += 1
    edge[...] = gathered
    for e in range(3):
        edge_copy(e).start()

    def mix(q, h, last, step, other_last, other_step, at):
        before = last - step
        share = 1.0 / (before * other_step + step * other_last)
        ratio = other_last * share / before
        if q:
            share = jnp.where(window == 0, share, 0.0)
            ratio = jnp.where(window == 0, ratio, 0.0)
        mixed[at, q, h, 0] = ratio
        mixed[at, q, h, 1] = share

    for e in range(3):
        pivot_copy(e).wait_recv()
    for h in range(HALF):
        mix(0, h, pivots[0, h, 0], pivots[0, h, 1], pivots_in[1, h, 0], pivots_in[1, h, 1], 0)
        if h < HALF - 1:
            mix(0, h, pivots_in[0, h, 0], pivots_in[0, h, 1], pivots_in[2, h, 0], pivots_in[2, h, 1], 1)

    first, final = lane == 0, lane == LANES - 1
    top, bottom = row == 0, row == ROWS - 1
    join_top = jnp.logical_and(top, jnp.logical_not(upper))
    join_bottom = jnp.logical_and(bottom, upper)
    join = jnp.logical_or(join_top, join_bottom)
    keep_up = jnp.where(top, zero, one)
    keep_down = jnp.where(bottom, zero, one)

    def spread(u, outside):
        lefts = [pltpu.roll(x, 1, 1) for x in u]
        rights = [pltpu.roll(x, LANES - 1, 1) for x in u]
        sums = []
        for q in range(2):
            up = keep_up * pltpu.roll(u[q], 1, 0)
            down = keep_down * pltpu.roll(u[q], ROWS - 1, 0)
            over = jnp.where(join, outside[q], zero)
            left = jnp.where(first, lefts[1 - q], lefts[q])
            right = jnp.where(final, rights[1 - q], rights[q])
            sums.append(((up + down) + over) + (left + right))
        return sums

    first_rows.wait_recv()
    ends = [zero] * 2
    ends_beyond = [zero] * 2
    for h in range(HALF):
        shift = shifts[h]
        if h == 1:
            for q in range(2):
                theta_copy(q).wait_recv()

        def forward(t, total, h=h, shift=shift, ends=ends, ends_beyond=ends_beyond):
            total = list(total)
            for s in range(UNROLL):
                k = t * UNROLL + s
                outside = [
                    jnp.broadcast_to(row_in[h, q, pl.ds(k, 1)], (ROWS, LANES)) for q in range(2)
                ]
                if h == 0:
                    u = [block[FIELD, q, k] for q in range(2)]
                else:
                    u = [theta[h - 1, q, k] * (state[q, k] + ends[q]) for q in range(2)]
                    outside = [
                        jnp.broadcast_to(theta_in[q, h - 1, pl.ds(k, 1)], (ROWS, LANES))
                        * (outside[q] + ends_beyond[q])
                        for q in range(2)
                    ]
                beside = spread(u, outside)
                for q in range(2):
                    flux = block[PLANE, q, k] * (beside[q] - 4.0 * u[q]) + block[SOURCE, q, k]
                    explicit = u[q] + shift * flux
                    total[q] = total[q] + weight[h, q, k] * explicit
                    state[q, k] = inverse[h, q, k] * total[q]
            return tuple(total)

        total = lax.fori_loop(0, layers // UNROLL, forward, (zero,) * 2)
        for q in range(2):
            planes[h, q] = total[q]
        targets = range(3) if h < HALF - 1 else (1,)
        for e in targets:
            plane_copy(h, e).start()

        def backward(t, later, h=h):
            later = list(later)
            for s in range(UNROLL):
                k = layers - 1 - (t * UNROLL + s)
                for q in range(2):
                    here = state[q, k]
                    if s == 0:
                        here = jnp.where(t == 0, zero, here)
                    later[q] = later[q] + here
                    state[q, k] = later[q]
                    if h < HALF - 1:
                        row_out[h + 1, q, pl.ds(k, 1)] = facing(later[q])[0:1]
            return tuple(later)

        lax.fori_loop(0, layers // UNROLL, backward, (zero,) * 2)
        if h < HALF - 1:
            row_copy(h + 1).start()
        if h == 0:
            for e in range(3):
                edge_copy(e).wait_recv()

            def pair(tile, i):
                both = [
                    pltpu.roll(tile, (LANES - 8 * c) % LANES, 1) if c else tile
                    for c in (2 * i, 2 * i + 1)
                ]
                return [jnp.where(window == 0, x, 1.0) for x in both]

            for i in range(HALF):
                mix(1, i, pivots[1, i, 0], pivots[1, i, 1], *pair(edge_in[1], i), 0)
                if i < HALF - 1:
                    mix(1, i, *pair(edge_in[0], i), *pair(edge_in[2], i), 1)
        for e in targets:
            plane_copy(h, e).wait_recv()
        ends = [
            mixed[0, q, h, 0] * total[q] + mixed[0, q, h, 1] * planes_in[h, 1, q] for q in range(2)
        ]
        if h < HALF - 1:
            ends_beyond = [
                beyond(
                    mixed[1, q, h, 0] * planes_in[h, 0, q] + mixed[1, q, h, 1] * planes_in[h, 2, q]
                )
                for q in range(2)
            ]
            row_copy(h + 1).wait_recv()

    def finish(t, _):
        for s in range(UNROLL):
            k = t * UNROLL + s
            result[layer(k)] = theta[HALF - 1, 0, k] * (state[0, k] + ends[0])
        return 0

    lax.fori_loop(0, layers // UNROLL, finish, 0)
    store = pltpu.make_async_copy(result, out_hbm, out_sem)
    store.start()

    for side, there in ((0, has_right), (1, has_left)):
        @pl.when(there)
        def _(side=side):
            far(side).wait_send()
            far_beside(side).wait_send()

    first_rows.wait_send()
    for e in range(3):
        pivot_copy(e).wait_send()
        edge_copy(e).wait_send()
    for q in range(2):
        theta_copy(q).wait_send()
    for h in range(HALF):
        for e in range(3) if h < HALF - 1 else (1,):
            plane_copy(h, e).wait_send()
        if h:
            row_copy(h).wait_send()
    store.wait()


def on_device(columns, field, plane, line, source, table, index):
    layers = field.shape[0]
    tile = (ROWS, LANES)
    f32 = jnp.float32
    groups = layers // 32
    dma = pltpu.SemaphoreType.DMA
    return pl.pallas_call(
        functools.partial(kernel, columns),
        out_shape=jax.ShapeDtypeStruct(field.shape, f32),
        in_specs=[pl.BlockSpec(memory_space=pltpu.HBM)] * 6,
        out_specs=pl.BlockSpec(memory_space=pltpu.HBM),
        scratch_shapes=[
            pltpu.SMEM(table.shape, f32),
            pltpu.SMEM(index.shape, jnp.int32),
            pltpu.VMEM((4, layers, *tile), f32),
            pltpu.VMEM((4, 2, layers, *tile), f32),
            pltpu.VMEM((HALF, 2, layers, *tile), f32),
            pltpu.VMEM((HALF, 2, layers, *tile), f32),
            pltpu.VMEM((HALF, 2, layers, *tile), f32),
            pltpu.VMEM((2, layers, *tile), f32),
            pltpu.VMEM((2, 4 * groups, *tile), f32),
            pltpu.VMEM((2, 4 * groups, *tile), f32),
            pltpu.VMEM((2, groups, *tile), f32),
            pltpu.VMEM((HALF, 2, layers, LANES), f32),
            pltpu.VMEM((HALF, 2, layers, LANES), f32),
            pltpu.VMEM((2, HALF - 1, layers, LANES), f32),
            pltpu.VMEM((2, HALF - 1, layers, LANES), f32),
            pltpu.VMEM((2, HALF, 2, *tile), f32),
            pltpu.VMEM((3, HALF, 2, *tile), f32),
            pltpu.VMEM(tile, f32),
            pltpu.VMEM((3, *tile), f32),
            pltpu.VMEM((2, 2, HALF, 2, *tile), f32),
            pltpu.VMEM((HALF, 2, *tile), f32),
            pltpu.VMEM((HALF, 3, 2, *tile), f32),
            pltpu.VMEM((layers, *tile), f32),
            dma((4,)), dma((2,)), dma,
            dma((2,)), dma((2,)), dma((2,)), dma((2,)), dma((HALF,)), dma((HALF,)), dma((2,)), dma((2,)),
            dma((3,)), dma((3,)), dma((3,)), dma((3,)), dma((HALF, 3)), dma((HALF, 3)),
        ],
        compiler_params=pltpu.CompilerParams(
            collective_id=0, has_side_effects=True, vmem_limit_bytes=67043328
        ),
    )(field, plane, line, source, table, index)


def solution(mesh):
    spec = P("gz", "gx", "gy")
    return jax.shard_map(
        functools.partial(on_device, mesh.shape["gy"]),
        mesh=mesh,
        in_specs=(spec, spec, spec, spec, P(), P()),
        out_specs=spec,
        check_vma=False,
    )
```

```python
import functools
import jax
import jax.numpy as jnp
from jax import lax
from jax.experimental import pallas as pl
from jax.experimental.pallas import tpu as pltpu
from jax.sharding import PartitionSpec as P

HALF = 4
ROWS = 8
LANES = 128
UNROLL = 16
FIELD, PLANE, LINE, SOURCE = range(4)
MESH = pl.DeviceIdType.MESH


def kernel(
    columns,
    field_hbm, plane_hbm, line_hbm, source_hbm, table_hbm, index_hbm,
    out_hbm,
    table, index, raw, block, theta, weight, inverse, state, packed, halo, halo_beside,
    row_out, row_in, theta_out, theta_in,
    pivots, pivots_in, edge, edge_in, mixed, planes, planes_in, result,
    local_sem, scalar_sem, out_sem,
    far_send, far_recv, beside_send, beside_recv, row_send, row_recv, theta_send, theta_recv,
    pivot_send, pivot_recv, edge_send, edge_recv, plane_send, plane_recv,
):
    layers = field_hbm.shape[0]
    gz, gx, gy = lax.axis_index("gz"), lax.axis_index("gx"), lax.axis_index("gy")
    has_left, has_right = gy > 0, gy < columns - 1
    lane = lax.broadcasted_iota(jnp.int32, (ROWS, LANES), 1)
    row = lax.broadcasted_iota(jnp.int32, (ROWS, LANES), 0)
    zero = jnp.zeros((ROWS, LANES), jnp.float32)
    one = jnp.ones((ROWS, LANES), jnp.float32)
    upper = jnp.full((ROWS, LANES), gx, jnp.int32) == 0

    def layer(k):
        return gz * (layers - 1) + (1 - 2 * gz) * k

    peers = (
        {"gx": 1 - gx},
        {"gz": 1 - gz},
        {"gz": 1 - gz, "gx": 1 - gx},
    )

    def facing(tile):
        return jnp.where(upper, pltpu.roll(tile, 1, 0), tile)

    def beyond(tile):
        first = jnp.broadcast_to(tile[0:1], (ROWS, LANES))
        last = jnp.broadcast_to(tile[ROWS - 1 : ROWS], (ROWS, LANES))
        return jnp.where(upper, first, last)

    loads = [
        pltpu.make_async_copy(source, raw.at[a], local_sem.at[a])
        for a, source in enumerate((field_hbm, plane_hbm, line_hbm, source_hbm))
    ]
    scalars = [
        pltpu.make_async_copy(table_hbm, table, scalar_sem.at[0]),
        pltpu.make_async_copy(index_hbm, index, scalar_sem.at[1]),
    ]
    for copy in scalars + loads:
        copy.start()

    barrier = pltpu.get_barrier_semaphore()
    for peer in peers:
        pl.semaphore_signal(barrier, inc=1, device_id=peer, device_id_type=MESH)

    @pl.when(has_left)
    def _():
        pl.semaphore_signal(barrier, inc=1, device_id={"gy": gy - 1}, device_id_type=MESH)
        pl.semaphore_signal(
            barrier, inc=1, device_id={"gy": gy - 1, "gx": 1 - gx}, device_id_type=MESH
        )

    @pl.when(has_right)
    def _():
        pl.semaphore_signal(barrier, inc=1, device_id={"gy": gy + 1}, device_id_type=MESH)
        pl.semaphore_signal(
            barrier, inc=1, device_id={"gy": gy + 1, "gx": 1 - gx}, device_id_type=MESH
        )

    for copy in scalars:
        copy.wait()
    shifts = [jnp.full((ROWS, LANES), table[index[h]], jnp.float32) for h in range(HALF)]
    inverses = [1.0 / s for s in shifts]

    for copy in loads:
        copy.wait()

    def arrange(t, _):
        for s in range(UNROLL):
            k = t * UNROLL + s
            at = layer(k)
            for a in range(4):
                block[a, 0, k] = raw[a, at]
            row_out[0, 0, pl.ds(k, 1)] = facing(raw[FIELD, at])[0:1]
        return 0

    lax.fori_loop(0, layers // UNROLL, arrange, 0)

    slots = LANES // 8
    groups = layers // (2 * slots)

    def pack(j, _):
        for a in range(4):
            left, right = zero, zero
            for b in range(2):
                for i in range(slots):
                    p = 8 * i + 4 * b
                    moved = block[a, 0, j * 2 * slots + b * slots + i]
                    if p:
                        moved = pltpu.roll(moved, p, 1)
                    at = lane // 4
                    right = jnp.where(at == p // 4, moved, right)
                    left = jnp.where(at == (p // 4 - 1) % 32, moved, left)
            packed[0, a * groups + j] = left
            packed[1, a * groups + j] = right
        return 0

    lax.fori_loop(0, groups, pack, 0)

    for side, missing in ((0, jnp.logical_not(has_left)), (1, jnp.logical_not(has_right))):
        @pl.when(missing)
        def _(side=side):
            for a in range(4):
                for j in range(groups):
                    halo[side, a * groups + j] = one * 1000.0 if a == LINE else zero
            for j in range(groups):
                halo_beside[side, j] = zero

    def factor(q):
        def steps(t, carry):
            carry = list(carry)
            for s in range(UNROLL):
                k = t * UNROLL + s
                line = 1.0 / block[LINE, q, k]
                for h in range(HALF):
                    th, de = carry[2 * h], carry[2 * h + 1]
                    ratio = line * inverses[h]
                    w = ratio * th
                    de = de + w
                    new = th + de
                    theta[h, q, k] = th
                    weight[h, q, k] = w
                    inverse[h, q, k] = 1.0 / (new * th)
                    if h < HALF - 1:
                        theta_out[q, h, pl.ds(k, 1)] = facing(th)[0:1]
                    carry[2 * h], carry[2 * h + 1] = new, de
            return tuple(carry)

        end = lax.fori_loop(0, layers // UNROLL, steps, (one,) * (2 * HALF))
        for h in range(HALF):
            pivots[q, h, 0] = end[2 * h]
            pivots[q, h, 1] = end[2 * h + 1]

    factor(0)

    signals = 3 + 2 * has_left.astype(jnp.int32) + 2 * has_right.astype(jnp.int32)
    pl.semaphore_wait(barrier, signals)

    def far(side):
        return pltpu.make_async_remote_copy(
            src_ref=packed.at[side],
            dst_ref=halo.at[side],
            send_sem=far_send.at[side],
            recv_sem=far_recv.at[side],
            device_id={"gy": gy + 1 - 2 * side},
            device_id_type=MESH,
        )

    def far_beside(side):
        return pltpu.make_async_remote_copy(
            src_ref=packed.at[side, pl.ds(FIELD * groups, groups)],
            dst_ref=halo_beside.at[side],
            send_sem=beside_send.at[side],
            recv_sem=beside_recv.at[side],
            device_id={"gy": gy + 1 - 2 * side, "gx": 1 - gx},
            device_id_type=MESH,
        )

    for side, there in ((0, has_right), (1, has_left)):
        @pl.when(there)
        def _(side=side):
            far(side).start()
            far_beside(side).start()

    def to_peer(source, target, send, recv, e):
        return pltpu.make_async_remote_copy(
            src_ref=source,
            dst_ref=target,
            send_sem=send,
            recv_sem=recv,
            device_id=peers[e],
            device_id_type=MESH,
        )

    def pivot_copy(e):
        return to_peer(pivots.at[0], pivots_in.at[e], pivot_send.at[e], pivot_recv.at[e], e)

    def edge_copy(e):
        return to_peer(edge, edge_in.at[e], edge_send.at[e], edge_recv.at[e], e)

    def plane_copy(h, e):
        return to_peer(
            planes.at[h], planes_in.at[h, e], plane_send.at[h, e], plane_recv.at[h, e], e
        )

    def theta_copy(q):
        return to_peer(theta_out.at[q], theta_in.at[q], theta_send.at[q], theta_recv.at[q], 0)

    def row_copy(h):
        return to_peer(row_out.at[h], row_in.at[h], row_send.at[h], row_recv.at[h], 0)

    first_rows = to_peer(row_out.at[0, 0], row_in.at[0, 0], row_send.at[0], row_recv.at[0], 0)

    first_rows.start()
    for e in range(3):
        pivot_copy(e).start()
    theta_copy(0).start()

    for side, there in ((0, has_left), (1, has_right)):
        @pl.when(there)
        def _(side=side):
            far(side).wait_recv()
            far_beside(side).wait_recv()

    odd = lax.rem(lane // 4, 2) == 1

    def unpack(j, _):
        for a in range(4):
            left, right = halo[0, a * groups + j], halo[1, a * groups + j]
            for b in range(2):
                both = jnp.where(odd, right, left) if b else jnp.where(odd, left, right)
                for i in range(slots):
                    p = 8 * i + 4 * b
                    block[a, 1, j * 2 * slots + b * slots + i] = (
                        pltpu.roll(both, LANES - p, 1) if p else both
                    )
        left, right = halo_beside[0, j], halo_beside[1, j]
        for b in range(2):
            both = jnp.where(odd, right, left) if b else jnp.where(odd, left, right)
            both = jnp.where(upper, both, pltpu.roll(both, 1, 0))
            for i in range(slots):
                p = 8 * i + 4 * b
                moved = pltpu.roll(both, LANES - p, 1) if p else both
                row_in[0, 1, pl.ds(j * 2 * slots + b * slots + i, 1)] = moved[0:1]
        return 0

    lax.fori_loop(0, groups, unpack, 0)
    factor(1)
    theta_copy(1).start()
    window = lax.rem(lane + 4, LANES) // 8
    slot = 0
    gathered = zero
    for h in range(HALF):
        for c in range(2):
            moved = pivots[1, h, c]
            if slot:
                moved = pltpu.roll(moved, 8 * slot, 1)
            gathered = jnp.where(window == slot, moved, gathered)
            slot += 1
    edge[...] = gathered
    for e in range(3):
        edge_copy(e).start()

    def mix(q, h, last, step, other_last, other_step, at):
        before = last - step
        share = 1.0 / (before * other_step + step * other_last)
        ratio = other_last * share / before
        if q:
            share = jnp.where(window == 0, share, 0.0)
            ratio = jnp.where(window == 0, ratio, 0.0)
        mixed[at, q, h, 0] = ratio
        mixed[at, q, h, 1] = share

    for e in range(3):
        pivot_copy(e).wait_recv()
    for h in range(HALF):
        mix(0, h, pivots[0, h, 0], pivots[0, h, 1], pivots_in[1, h, 0], pivots_in[1, h, 1], 0)
        if h < HALF - 1:
            mix(0, h, pivots_in[0, h, 0], pivots_in[0, h, 1], pivots_in[2, h, 0], pivots_in[2, h, 1], 1)

    first, final = lane == 0, lane == LANES - 1
    top, bottom = row == 0, row == ROWS - 1
    join_top = jnp.logical_and(top, jnp.logical_not(upper))
    join_bottom = jnp.logical_and(bottom, upper)
    join = jnp.logical_or(join_top, join_bottom)
    keep_up = jnp.where(top, zero, one)
    keep_down = jnp.where(bottom, zero, one)

    def spread(u, outside):
        lefts = [pltpu.roll(x, 1, 1) for x in u]
        rights = [pltpu.roll(x, LANES - 1, 1) for x in u]
        sums = []
        for q in range(2):
            up = keep_up * pltpu.roll(u[q], 1, 0)
            down = keep_down * pltpu.roll(u[q], ROWS - 1, 0)
            over = jnp.where(join, outside[q], zero)
            left = jnp.where(first, lefts[1 - q], lefts[q])
            right = jnp.where(final, rights[1 - q], rights[q])
            sums.append(((up + down) + over) + (left + right))
        return sums

    first_rows.wait_recv()
    ends = [zero] * 2
    ends_beyond = [zero] * 2
    for h in range(HALF):
        shift = shifts[h]
        if h == 1:
            for q in range(2):
                theta_copy(q).wait_recv()

        def forward(t, total, h=h, shift=shift, ends=ends, ends_beyond=ends_beyond):
            total = list(total)
            for s in range(64):
                k = t * 64 + s
                outside = [
                    jnp.broadcast_to(row_in[h, q, pl.ds(k, 1)], (ROWS, LANES)) for q in range(2)
                ]
                if h == 0:
                    u = [block[FIELD, q, k] for q in range(2)]
                else:
                    u = [theta[h - 1, q, k] * (state[q, k] + ends[q]) for q in range(2)]
                    outside = [
                        jnp.broadcast_to(theta_in[q, h - 1, pl.ds(k, 1)], (ROWS, LANES))
                        * (outside[q] + ends_beyond[q])
                        for q in range(2)
                    ]
                beside = spread(u, outside)
                for q in range(2):
                    flux = block[PLANE, q, k] * (beside[q] - 4.0 * u[q]) + block[SOURCE, q, k]
                    explicit = u[q] + shift * flux
                    total[q] = total[q] + weight[h, q, k] * explicit
                    state[q, k] = inverse[h, q, k] * total[q]
            return tuple(total)

        total = lax.fori_loop(0, 1, forward, (zero,) * 2)
        for q in range(2):
            planes[h, q] = total[q]
        targets = range(3) if h < HALF - 1 else (1,)
        for e in targets:
            plane_copy(h, e).start()

        def backward(t, later, h=h):
            later = list(later)
            for s in range(UNROLL):
                k = layers - 1 - (t * UNROLL + s)
                for q in range(2):
                    here = state[q, k]
                    if s == 0:
                        here = jnp.where(t == 0, zero, here)
                    later[q] = later[q] + here
                    state[q, k] = later[q]
                    if h < HALF - 1:
                        row_out[h + 1, q, pl.ds(k, 1)] = facing(later[q])[0:1]
            return tuple(later)

        lax.fori_loop(0, layers // UNROLL, backward, (zero,) * 2)
        if h < HALF - 1:
            row_copy(h + 1).start()
        if h == 0:
            for e in range(3):
                edge_copy(e).wait_recv()

            def pair(tile, i):
                both = [
                    pltpu.roll(tile, (LANES - 8 * c) % LANES, 1) if c else tile
                    for c in (2 * i, 2 * i + 1)
                ]
                return [jnp.where(window == 0, x, 1.0) for x in both]

            for i in range(HALF):
                mix(1, i, pivots[1, i, 0], pivots[1, i, 1], *pair(edge_in[1], i), 0)
                if i < HALF - 1:
                    mix(1, i, *pair(edge_in[0], i), *pair(edge_in[2], i), 1)
        for e in targets:
            plane_copy(h, e).wait_recv()
        ends = [
            mixed[0, q, h, 0] * total[q] + mixed[0, q, h, 1] * planes_in[h, 1, q] for q in range(2)
        ]
        if h < HALF - 1:
            ends_beyond = [
                beyond(
                    mixed[1, q, h, 0] * planes_in[h, 0, q] + mixed[1, q, h, 1] * planes_in[h, 2, q]
                )
                for q in range(2)
            ]
            row_copy(h + 1).wait_recv()

    def finish(t, _):
        for s in range(UNROLL):
            k = t * UNROLL + s
            result[layer(k)] = theta[HALF - 1, 0, k] * (state[0, k] + ends[0])
        return 0

    lax.fori_loop(0, layers // UNROLL, finish, 0)
    store = pltpu.make_async_copy(result, out_hbm, out_sem)
    store.start()

    for side, there in ((0, has_right), (1, has_left)):
        @pl.when(there)
        def _(side=side):
            far(side).wait_send()
            far_beside(side).wait_send()

    first_rows.wait_send()
    for e in range(3):
        pivot_copy(e).wait_send()
        edge_copy(e).wait_send()
    for q in range(2):
        theta_copy(q).wait_send()
    for h in range(HALF):
        for e in range(3) if h < HALF - 1 else (1,):
            plane_copy(h, e).wait_send()
        if h:
            row_copy(h).wait_send()
    store.wait()


def on_device(columns, field, plane, line, source, table, index):
    layers = field.shape[0]
    tile = (ROWS, LANES)
    f32 = jnp.float32
    groups = layers // 32
    dma = pltpu.SemaphoreType.DMA
    return pl.pallas_call(
        functools.partial(kernel, columns),
        out_shape=jax.ShapeDtypeStruct(field.shape, f32),
        in_specs=[pl.BlockSpec(memory_space=pltpu.HBM)] * 6,
        out_specs=pl.BlockSpec(memory_space=pltpu.HBM),
        scratch_shapes=[
            pltpu.SMEM(table.shape, f32),
            pltpu.SMEM(index.shape, jnp.int32),
            pltpu.VMEM((4, layers, *tile), f32),
            pltpu.VMEM((4, 2, layers, *tile), f32),
            pltpu.VMEM((HALF, 2, layers, *tile), f32),
            pltpu.VMEM((HALF, 2, layers, *tile), f32),
            pltpu.VMEM((HALF, 2, layers, *tile), f32),
            pltpu.VMEM((2, layers, *tile), f32),
            pltpu.VMEM((2, 4 * groups, *tile), f32),
            pltpu.VMEM((2, 4 * groups, *tile), f32),
            pltpu.VMEM((2, groups, *tile), f32),
            pltpu.VMEM((HALF, 2, layers, LANES), f32),
            pltpu.VMEM((HALF, 2, layers, LANES), f32),
            pltpu.VMEM((2, HALF - 1, layers, LANES), f32),
            pltpu.VMEM((2, HALF - 1, layers, LANES), f32),
            pltpu.VMEM((2, HALF, 2, *tile), f32),
            pltpu.VMEM((3, HALF, 2, *tile), f32),
            pltpu.VMEM(tile, f32),
            pltpu.VMEM((3, *tile), f32),
            pltpu.VMEM((2, 2, HALF, 2, *tile), f32),
            pltpu.VMEM((HALF, 2, *tile), f32),
            pltpu.VMEM((HALF, 3, 2, *tile), f32),
            pltpu.VMEM((layers, *tile), f32),
            dma((4,)), dma((2,)), dma,
            dma((2,)), dma((2,)), dma((2,)), dma((2,)), dma((HALF,)), dma((HALF,)), dma((2,)), dma((2,)),
            dma((3,)), dma((3,)), dma((3,)), dma((3,)), dma((HALF, 3)), dma((HALF, 3)),
        ],
        compiler_params=pltpu.CompilerParams(
            collective_id=0, has_side_effects=True, vmem_limit_bytes=67043328
        ),
    )(field, plane, line, source, table, index)


def solution(mesh):
    spec = P("gz", "gx", "gy")
    return jax.shard_map(
        functools.partial(on_device, mesh.shape["gy"]),
        mesh=mesh,
        in_specs=(spec, spec, spec, spec, P(), P()),
        out_specs=spec,
        check_vma=False,
    )
```

```python
import functools
import jax
import jax.numpy as jnp
from jax import lax
from jax.experimental import pallas as pl
from jax.experimental.pallas import tpu as pltpu
from jax.sharding import PartitionSpec as P

HALF = 4
ROWS = 8
LANES = 128
UNROLL = 16
SPAN = 64
FIELD, PLANE, LINE, SOURCE = range(4)
MESH = pl.DeviceIdType.MESH


def turn(tile, shift):
    shift %= LANES
    return pltpu.roll(tile, shift, 1) if shift else tile


def kernel(
    columns,
    field_hbm, plane_hbm, line_hbm, source_hbm, table_hbm, index_hbm,
    out_hbm,
    table, index, raw, block, swapped, theta, weight, inverse, state,
    far_out, far_in, near_out, near_in, far_turned, near_turned, far_merged, near_merged, strip_out, strip_in, strip_end,
    row_out, row_in, theta_out, theta_in,
    pivots, pivots_in, mixed, planes, planes_in, result,
    local_sem, scalar_sem, out_sem,
    far_send, far_recv, near_send, near_recv, swap_send, swap_recv, strip_send, strip_recv,
    row_send, row_recv, theta_send, theta_recv, pivot_send, pivot_recv, plane_send, plane_recv,
):
    layers = field_hbm.shape[0]
    gz, gx, gy = lax.axis_index("gz"), lax.axis_index("gx"), lax.axis_index("gy")
    has_left, has_right = gy > 0, gy < columns - 1
    solver = gx == 1
    wants_left = jnp.logical_and(solver, jnp.logical_and(gz == 0, has_left))
    wants_right = jnp.logical_and(solver, jnp.logical_and(gz == 1, has_right))
    lacks = jnp.logical_and(
        solver, jnp.logical_not(jnp.logical_or(wants_left, wants_right))
    )
    lane = lax.broadcasted_iota(jnp.int32, (ROWS, LANES), 1)
    row = lax.broadcasted_iota(jnp.int32, (ROWS, LANES), 0)
    zero = jnp.zeros((ROWS, LANES), jnp.float32)
    one = jnp.ones((ROWS, LANES), jnp.float32)
    upper = jnp.full((ROWS, LANES), gx, jnp.int32) == 0
    half = LANES // 2

    def part(offset, size):
        return lax.rem(lane - offset + LANES, LANES) // size

    def layer(k):
        return gz * (layers - 1) + (1 - 2 * gz) * k

    peers = (
        {"gx": 1 - gx},
        {"gz": 1 - gz},
        {"gz": 1 - gz, "gx": 1 - gx},
    )

    def facing(tile):
        return jnp.where(upper, pltpu.roll(tile, 1, 0), tile)

    def beyond(tile):
        first = jnp.broadcast_to(tile[0:1], (ROWS, LANES))
        last = jnp.broadcast_to(tile[ROWS - 1 : ROWS], (ROWS, LANES))
        return jnp.where(upper, first, last)

    loads = [
        pltpu.make_async_copy(source, raw.at[a], local_sem.at[a])
        for a, source in enumerate((field_hbm, plane_hbm, line_hbm, source_hbm))
    ]
    scalars = [
        pltpu.make_async_copy(table_hbm, table, scalar_sem.at[0]),
        pltpu.make_async_copy(index_hbm, index, scalar_sem.at[1]),
    ]
    for copy in scalars + loads:
        copy.start()

    barrier = pltpu.get_barrier_semaphore()
    beside = ({}, {"gx": 1 - gx}, {"gz": 1 - gz}, {"gz": 1 - gz, "gx": 1 - gx})
    for step, there in ((-1, has_left), (1, has_right)):
        @pl.when(there)
        def _(step=step):
            for other in beside:
                pl.semaphore_signal(
                    barrier, inc=1, device_id={"gy": gy + step, **other}, device_id_type=MESH
                )

    for peer in peers:
        pl.semaphore_signal(barrier, inc=1, device_id=peer, device_id_type=MESH)

    for copy in scalars:
        copy.wait()
    shifts = [jnp.full((ROWS, LANES), table[index[h]], jnp.float32) for h in range(HALF)]
    inverses = [1.0 / s for s in shifts]

    for copy in loads:
        copy.wait()

    def arrange(t, _):
        for s in range(UNROLL):
            k = t * UNROLL + s
            at = layer(k)
            for a in range(4):
                block[a, 0, k] = raw[a, at]
            row_out[0, pl.ds(k, 1)] = facing(raw[FIELD, at])[0:1]
        return 0

    lax.fori_loop(0, layers // UNROLL, arrange, 0)

    slots = LANES // 8
    groups = layers // (2 * slots)

    def pack(j, _):
        at = lane // 4
        for a in range(4):
            left, right = zero, zero
            for b in range(2):
                near = zero
                near_slot = part(4 * b - 8 + 8 * gz, 8)
                for i in range(slots):
                    p = 8 * i + 4 * b
                    moved = turn(block[a, 0, j * 2 * slots + b * slots + i], p)
                    right = jnp.where(at == p // 4, moved, right)
                    left = jnp.where(at == (p // 4 - 1) % 32, moved, left)
                    near = jnp.where(near_slot == i, moved, near)
                near_out[a * 2 * groups + 2 * j + b] = near
            far_out[0, a * groups + j] = left
            far_out[1, a * groups + j] = right
        return 0

    lax.fori_loop(0, groups, pack, 0)

    @pl.when(lacks)
    def _():
        for q in range(4):
            for a in range(4):
                for j in range(groups):
                    far_in[q, a * groups + j] = one * 1000.0 if a == LINE else zero

    def factor(q):
        def steps(t, carry):
            carry = list(carry)
            for s in range(UNROLL):
                k = t * UNROLL + s
                line = 1.0 / block[LINE, q, k]
                for h in range(HALF):
                    th, de = carry[2 * h], carry[2 * h + 1]
                    ratio = line * inverses[h]
                    w = ratio * th
                    de = de + w
                    new = th + de
                    theta[h, q, k] = th
                    weight[h, q, k] = w
                    inverse[h, q, k] = 1.0 / (new * th)
                    if q == 0 and h < HALF - 1:
                        theta_out[h, pl.ds(k, 1)] = facing(th)[0:1]
                    carry[2 * h], carry[2 * h + 1] = new, de
            return tuple(carry)

        return lax.fori_loop(0, layers // UNROLL, steps, (one,) * (2 * HALF))

    @pl.when(solver)
    def _():
        def shift_own(t, _):
            for s in range(UNROLL):
                k = t * UNROLL + s
                for a in range(4):
                    block[a, 1, k] = turn(block[a, 0, k], 32)
            return 0

        lax.fori_loop(0, layers // UNROLL, shift_own, 0)

    found = factor(0)
    for h in range(HALF):
        pivots[h, 0] = found[2 * h]
        pivots[h, 1] = found[2 * h + 1]

    pl.semaphore_wait(barrier, 3 + 4 * has_left.astype(jnp.int32) + 4 * has_right.astype(jnp.int32))

    def send(source, target, send_sem, recv_sem, device):
        return pltpu.make_async_remote_copy(
            src_ref=source,
            dst_ref=target,
            send_sem=send_sem,
            recv_sem=recv_sem,
            device_id=device,
            device_id_type=MESH,
        )

    from_left = 2 * gz + gx
    from_right = 2 * (1 - gz) + gx

    def far(way, quarter):
        device = {"gy": gy + 1 - 2 * way}
        if quarter // 2:
            device["gz"] = 1 - gz
        if quarter % 2 == 0:
            device["gx"] = 1 - gx
        return send(
            far_out.at[way], far_in.at[quarter], far_send.at[way], far_recv.at[quarter], device
        )

    def far_arrival(quarter):
        return send(
            far_out.at[0], far_in.at[quarter], far_send.at[0], far_recv.at[quarter], peers[0]
        )

    def near(x):
        return send(near_out, near_in.at[x], near_send, near_recv.at[x], {"gz": 1 - gz, "gx": 1})

    def near_arrival(x):
        return send(near_out, near_in.at[x], near_send, near_recv.at[x], peers[1])

    def swap(a):
        return send(
            block.at[a, 0], swapped.at[a], swap_send.at[a], swap_recv.at[a], {"gx": 1 - gx}
        )

    def pivot_copy(e):
        return send(pivots, pivots_in.at[e], pivot_send.at[e], pivot_recv.at[e], peers[e])

    def plane_copy(h, e):
        return send(
            planes.at[h], planes_in.at[h, e], plane_send.at[h, e], plane_recv.at[h, e], peers[e]
        )

    def row_copy(h):
        rows = pl.ds(0, layers)
        return send(
            row_out.at[h, rows], row_in.at[h, rows], row_send.at[h], row_recv.at[h], peers[0]
        )

    every = (pl.ds(0, HALF - 1), pl.ds(0, layers))
    theta_copy = send(theta_out.at[every], theta_in.at[every], theta_send, theta_recv, peers[0])

    def strip_copy(e, side):
        return send(
            strip_out, strip_in.at[side], strip_send.at[e], strip_recv.at[side], peers[e]
        )

    def strip_arrival(side):
        return send(
            strip_out, strip_in.at[side], strip_send.at[0], strip_recv.at[side], peers[0]
        )

    row_copy(0).start()
    for way, there, place in ((0, has_right, from_left), (1, has_left, from_right)):
        @pl.when(there)
        def _(way=way, place=place):
            for quarter in range(4):
                @pl.when(place == quarter)
                def _(quarter=quarter):
                    far(way, quarter).start()

    for e in range(3):
        pivot_copy(e).start()
    for x in range(2):
        @pl.when(gx == x)
        def _(x=x):
            near(x).start()

    theta_copy.start()

    @pl.when(gx == 0)
    def _():
        for a in range(4):
            swap(a).start()

    top, bottom = row == 0, row == ROWS - 1
    join = jnp.logical_or(
        jnp.logical_and(top, jnp.logical_not(upper)), jnp.logical_and(bottom, upper)
    )
    keep_up = jnp.where(top, zero, one)
    keep_down = jnp.where(bottom, zero, one)
    keep_left = jnp.where(lane == 0, zero, one)
    keep_right = jnp.where(lane == LANES - 1, zero, one)

    def spread(u, outside):
        up = keep_up * pltpu.roll(u, 1, 0)
        down = keep_down * pltpu.roll(u, ROWS - 1, 0)
        over = jnp.where(join, outside, zero)
        left = keep_left * turn(u, 1)
        right = keep_right * turn(u, -1)
        return ((up + down) + over) + (left + right)

    region = part(-8, 32)
    lower_rows = lax.rem(region, 2) == 1
    cross_up = jnp.logical_and(top, lower_rows)
    cross_down = jnp.logical_and(bottom, jnp.logical_not(lower_rows))

    def strip_spread(u):
        above, below = pltpu.roll(u, 1, 0), pltpu.roll(u, ROWS - 1, 0)
        up = jnp.where(cross_up, turn(above, 32), keep_up * above)
        down = jnp.where(cross_down, turn(below, -32), keep_down * below)
        return (up + down) + (turn(u, 1) + turn(u, -1))

    def eliminate(h, q, values):
        shift = shifts[h]

        def forward(t, total):
            for s in range(SPAN):
                k = t * SPAN + s
                u, beside = values(k)
                flux = block[PLANE, q, k] * (beside - 4.0 * u) + block[SOURCE, q, k]
                total = total + weight[h, q, k] * (u + shift * flux)
                state[q, k] = inverse[h, q, k] * total
            return total

        return lax.fori_loop(0, layers // SPAN, forward, zero)

    def substitute(h, q):
        def backward(t, later):
            for s in range(UNROLL):
                k = layers - 1 - (t * UNROLL + s)
                here = state[q, k]
                if s == 0:
                    here = jnp.where(t == 0, zero, here)
                later = later + here
                state[q, k] = later
                if q == 0 and h < HALF - 1:
                    row_out[h + 1, pl.ds(k, 1)] = facing(later)[0:1]
            return later

        lax.fori_loop(0, layers // UNROLL, backward, zero)

    def targets(h):
        return range(3) if h < HALF - 1 else (1,)

    now = {}

    def run(h):
        end, end_beyond = now.get("end"), now.get("beyond")

        def values(k):
            outside = jnp.broadcast_to(row_in[h, pl.ds(k, 1)], (ROWS, LANES))
            if h == 0:
                u = block[FIELD, 0, k]
            else:
                u = theta[h - 1, 0, k] * (state[0, k] + end)
                outside = jnp.broadcast_to(theta_in[h - 1, pl.ds(k, 1)], (ROWS, LANES)) * (
                    outside + end_beyond
                )
            return u, spread(u, outside)

        total = eliminate(h, 0, values)
        now["total"] = total
        planes[h] = total
        for e in targets(h):
            plane_copy(h, e).start()
        substitute(h, 0)
        if h < HALF - 1:
            row_copy(h + 1).start()

    def settle(h):
        for e in targets(h):
            plane_copy(h, e).wait_recv()
        now["end"] = mixed[0, h, 0] * now["total"] + mixed[0, h, 1] * planes_in[h, 1]
        if h < HALF - 1:
            now["beyond"] = beyond(
                mixed[1, h, 0] * planes_in[h, 0] + mixed[1, h, 1] * planes_in[h, 2]
            )
            row_copy(h + 1).wait_recv()

    def mix(at, h, last, step, other_last, other_step):
        before = last - step
        share = 1.0 / (before * other_step + step * other_last)
        mixed[at, h, 0] = other_last * share / before
        mixed[at, h, 1] = share

    def merge(source, turned, merged, count, quarters):
        for d in range(4):
            for q in range(count):
                for at in range(source.shape[1]):
                    turned[d, q, at] = turn(source[q, at], 32 * d)
        for b in range(2):
            pick = quarters(b)
            for a in range(4):
                for j in range(groups):
                    at = a * groups + j
                    if count == 2:
                        at = a * 2 * groups + 2 * j + b
                    for m in range(4):
                        tiles = [turned[(4 - count + q - m) % 4, q, at] for q in range(count)]
                        tile = tiles[-1]
                        for q in range(count - 1):
                            tile = jnp.where(pick == 4 - count + q, tiles[q], tile)
                        merged[b, (a * groups + j) * 4 + m] = tile

    def strip_near():
        for a in range(4):
            swap(a).wait_recv()
        for x in range(2):
            near_arrival(x).wait_recv()
        merge(near_in, near_turned, near_merged, 2, lambda b: part(4 * b - 8 * gz, 32))

    def strip_far():
        @pl.when(jnp.logical_or(wants_left, wants_right))
        def _():
            for q in range(4):
                far_arrival(q).wait_recv()

        merge(far_in, far_turned, far_merged, 4, lambda b: part(4 * b - 4 + 4 * gz, 32))
        outer = lax.rem(lane + 4 - 4 * gz, 32) < 4

        for n in range(8):
            def gather(j, _, n=n):
                for a in range(4):
                    for m in range(4):
                        at = (a * groups + j) * 4 + m
                        k = j * 2 * slots + 4 * m + n % 2 * slots + n // 2
                        there = turn(near_merged[n % 2, at], -4 * n)
                        tile = turn(far_merged[n % 2, at], -4 * n)
                        own = jnp.where(region == 0, swapped[a, k], block[a, 1, k])
                        own = jnp.where(region < 2, own, there)
                        block[a, 1, k] = jnp.where(outer, tile, own)
                return 0

            lax.fori_loop(0, groups, gather, 0)

        ends = factor(1)
        for h in range(HALF):
            last, step = ends[2 * h], ends[2 * h + 1]
            mix(2, h, last, step, turn(last, half), turn(step, half))

    def strip_run(h):
        end = strip_end[...] if h else None

        def values(k):
            u = theta[h - 1, 1, k] * (state[1, k] + end) if h else block[FIELD, 1, k]
            return u, strip_spread(u)

        total = eliminate(h, 1, values)
        substitute(h, 1)
        strip_end[...] = mixed[2, h, 0] * total + mixed[2, h, 1] * turn(total, half)

    def strip_share():
        end = strip_end[...]
        slot = lax.rem(lane + 4 * gz, 32) // 4

        tiles = [zero] * (layers // 8)
        for i in range(8):
            for v in range(layers // 8):
                k = v * 8 + i
                moved = turn(theta[HALF - 1, 1, k] * (state[1, k] + end), 4 * i)
                tiles[v] = jnp.where(slot == i, moved, tiles[v])
        for v in range(layers // 8):
            strip_out[v] = tiles[v]
        for side in range(2):
            @pl.when(gz == side)
            def _(side=side):
                for e in (1, 2, 0):
                    strip_copy(e, side).start()
                for v in range(layers // 8):
                    strip_in[side, v] = tiles[v]

    row_copy(0).wait_recv()
    run(0)
    for e in range(3):
        pivot_copy(e).wait_recv()
    for h in range(HALF):
        mix(0, h, pivots[h, 0], pivots[h, 1], pivots_in[1, h, 0], pivots_in[1, h, 1])
        if h < HALF - 1:
            mix(1, h, pivots_in[0, h, 0], pivots_in[0, h, 1], pivots_in[2, h, 0], pivots_in[2, h, 1])
    settle(0)
    theta_copy.wait_recv()
    run(1)

    @pl.when(solver)
    def _():
        strip_near()
        strip_far()
        strip_run(0)

    settle(1)
    run(2)

    @pl.when(solver)
    def _():
        strip_run(1)
        strip_run(2)
        strip_run(3)
        strip_share()

    settle(2)
    run(3)

    settle(3)
    end = now["end"]

    @pl.when(jnp.logical_or(gx == 0, gz == 1))
    def _():
        strip_arrival(0).wait_recv()

    @pl.when(jnp.logical_or(gx == 0, gz == 0))
    def _():
        strip_arrival(1).wait_recv()

    lower_core = jnp.full((ROWS, LANES), gx, jnp.int32) == 1
    for side in range(2):
        other_half = jnp.full((ROWS, LANES), gz, jnp.int32) != side
        for v in range(layers // 8):
            tile = strip_in[side, v]
            tile = jnp.where(other_half, turn(tile, half), tile)
            strip_in[side, v] = jnp.where(lower_core, turn(tile, -32), tile)

    for i in range(8):
        for v in range(layers // 8):
            k = v * 8 + i
            left = turn(strip_in[0, v], -4 * i)
            right = turn(strip_in[1, v], -4 * i)
            inner = theta[HALF - 1, 0, k] * (state[0, k] + end)
            inner = jnp.where(lane < 4, left, inner)
            result[layer(k)] = jnp.where(lane >= LANES - 4, right, inner)
    store = pltpu.make_async_copy(result, out_hbm, out_sem)
    store.start()

    for way, there in ((0, has_right), (1, has_left)):
        @pl.when(there)
        def _(way=way):
            far(way, 0).wait_send()

    @pl.when(gx == 0)
    def _():
        for a in range(4):
            swap(a).wait_send()

    @pl.when(solver)
    def _():
        for e in range(3):
            strip_copy(e, 0).wait_send()

    near(0).wait_send()
    theta_copy.wait_send()
    for e in range(3):
        pivot_copy(e).wait_send()
    for h in range(HALF):
        row_copy(h).wait_send()
        for e in targets(h):
            plane_copy(h, e).wait_send()
    store.wait()


def on_device(columns, field, plane, line, source, table, index):
    layers = field.shape[0]
    tile = (ROWS, LANES)
    f32 = jnp.float32
    groups = layers // 32
    dma = pltpu.SemaphoreType.DMA
    return pl.pallas_call(
        functools.partial(kernel, columns),
        out_shape=jax.ShapeDtypeStruct(field.shape, f32),
        in_specs=[pl.BlockSpec(memory_space=pltpu.HBM)] * 6,
        out_specs=pl.BlockSpec(memory_space=pltpu.HBM),
        scratch_shapes=[
            pltpu.SMEM(table.shape, f32),
            pltpu.SMEM(index.shape, jnp.int32),
            pltpu.VMEM((4, layers, *tile), f32),
            pltpu.VMEM((4, 2, layers, *tile), f32),
            pltpu.VMEM((4, layers, *tile), f32),
            pltpu.VMEM((HALF, 2, layers, *tile), f32),
            pltpu.VMEM((HALF, 2, layers, *tile), f32),
            pltpu.VMEM((HALF, 2, layers, *tile), f32),
            pltpu.VMEM((2, layers, *tile), f32),
            pltpu.VMEM((2, 4 * groups, *tile), f32),
            pltpu.VMEM((4, 4 * groups, *tile), f32),
            pltpu.VMEM((8 * groups, *tile), f32),
            pltpu.VMEM((2, 8 * groups, *tile), f32),
            pltpu.VMEM((4, 4, 4 * groups, *tile), f32),
            pltpu.VMEM((4, 2, 8 * groups, *tile), f32),
            pltpu.VMEM((2, 16 * groups, *tile), f32),
            pltpu.VMEM((2, 16 * groups, *tile), f32),
            pltpu.VMEM((layers // 8, *tile), f32),
            pltpu.VMEM((2, layers // 8, *tile), f32),
            pltpu.VMEM(tile, f32),
            pltpu.VMEM((HALF, layers + ROWS, LANES), f32),
            pltpu.VMEM((HALF, layers + ROWS, LANES), f32),
            pltpu.VMEM((HALF - 1, layers + ROWS, LANES), f32),
            pltpu.VMEM((HALF - 1, layers + ROWS, LANES), f32),
            pltpu.VMEM((HALF, 2, *tile), f32),
            pltpu.VMEM((3, HALF, 2, *tile), f32),
            pltpu.VMEM((3, HALF, 2, *tile), f32),
            pltpu.VMEM((HALF, *tile), f32),
            pltpu.VMEM((HALF, 3, *tile), f32),
            pltpu.VMEM((layers, *tile), f32),
            dma((4,)), dma((2,)), dma,
            dma((2,)), dma((4,)), dma, dma((2,)), dma((4,)), dma((4,)), dma((3,)), dma((2,)),
            dma((HALF,)), dma((HALF,)), dma, dma, dma((3,)), dma((3,)), dma((HALF, 3)), dma((HALF, 3)),
        ],
        compiler_params=pltpu.CompilerParams(
            collective_id=0, has_side_effects=True, vmem_limit_bytes=67043328
        ),
    )(field, plane, line, source, table, index)


def solution(mesh):
    spec = P("gz", "gx", "gy")
    return jax.shard_map(
        functools.partial(on_device, mesh.shape["gy"]),
        mesh=mesh,
        in_specs=(spec, spec, spec, spec, P(), P()),
        out_specs=spec,
        check_vma=False,
    )
```

```python
import functools
import jax
import jax.numpy as jnp
from jax import lax
from jax.experimental import pallas as pl
from jax.experimental.pallas import tpu as pltpu
from jax.sharding import PartitionSpec as P

HALF = 4
ROWS = 8
LANES = 128
UNROLL = 16
SPAN = 64
FIELD, PLANE, LINE, SOURCE = range(4)
MESH = pl.DeviceIdType.MESH


def turn(tile, shift):
    shift %= LANES
    return pltpu.roll(tile, shift, 1) if shift else tile


def kernel(
    columns,
    field_hbm, plane_hbm, line_hbm, source_hbm, table_hbm, index_hbm,
    out_hbm,
    table, index, raw, block, swapped, theta, weight, inverse, state,
    far_out, far_in, near_out, near_in, far_turned, near_turned, far_merged, near_merged, strip_out, strip_in, strip_end,
    row_out, row_in, theta_out, theta_in,
    pivots, pivots_in, mixed, planes, planes_in, result,
    local_sem, scalar_sem, out_sem,
    far_send, far_recv, near_send, near_recv, swap_send, swap_recv, strip_send, strip_recv,
    row_send, row_recv, theta_send, theta_recv, pivot_send, pivot_recv, plane_send, plane_recv,
):
    layers = field_hbm.shape[0]
    gz, gx, gy = lax.axis_index("gz"), lax.axis_index("gx"), lax.axis_index("gy")
    has_left, has_right = gy > 0, gy < columns - 1
    solver = gx == 1
    wants_left = jnp.logical_and(solver, jnp.logical_and(gz == 0, has_left))
    wants_right = jnp.logical_and(solver, jnp.logical_and(gz == 1, has_right))
    lacks = jnp.logical_and(
        solver, jnp.logical_not(jnp.logical_or(wants_left, wants_right))
    )
    lane = lax.broadcasted_iota(jnp.int32, (ROWS, LANES), 1)
    row = lax.broadcasted_iota(jnp.int32, (ROWS, LANES), 0)
    zero = jnp.zeros((ROWS, LANES), jnp.float32)
    one = jnp.ones((ROWS, LANES), jnp.float32)
    upper = jnp.full((ROWS, LANES), gx, jnp.int32) == 0
    half = LANES // 2

    def part(offset, size):
        return lax.rem(lane - offset + LANES, LANES) // size

    def layer(k):
        return gz * (layers - 1) + (1 - 2 * gz) * k

    peers = (
        {"gx": 1 - gx},
        {"gz": 1 - gz},
        {"gz": 1 - gz, "gx": 1 - gx},
    )

    def facing(tile):
        return jnp.where(upper, pltpu.roll(tile, 1, 0), tile)

    def beyond(tile):
        first = jnp.broadcast_to(tile[0:1], (ROWS, LANES))
        last = jnp.broadcast_to(tile[ROWS - 1 : ROWS], (ROWS, LANES))
        return jnp.where(upper, first, last)

    loads = [
        pltpu.make_async_copy(source, raw.at[a], local_sem.at[a])
        for a, source in enumerate((field_hbm, plane_hbm, line_hbm, source_hbm))
    ]
    scalars = [
        pltpu.make_async_copy(table_hbm, table, scalar_sem.at[0]),
        pltpu.make_async_copy(index_hbm, index, scalar_sem.at[1]),
    ]
    for copy in scalars + loads:
        copy.start()

    barrier = pltpu.get_barrier_semaphore()
    beside = ({}, {"gx": 1 - gx}, {"gz": 1 - gz}, {"gz": 1 - gz, "gx": 1 - gx})
    for step, wanted in ((-1, wants_left), (1, wants_right)):
        @pl.when(wanted)
        def _(step=step):
            for other in beside:
                pl.semaphore_signal(
                    barrier, inc=1, device_id={"gy": gy + step, **other}, device_id_type=MESH
                )

    for peer in peers:
        pl.semaphore_signal(barrier, inc=1, device_id=peer, device_id_type=MESH)

    for copy in scalars:
        copy.wait()
    shifts = [jnp.full((ROWS, LANES), table[index[h]], jnp.float32) for h in range(HALF)]
    inverses = [1.0 / s for s in shifts]

    for copy in loads:
        copy.wait()

    def arrange(t, _):
        for s in range(UNROLL):
            k = t * UNROLL + s
            at = layer(k)
            for a in range(4):
                block[a, 0, k] = raw[a, at]
            row_out[0, pl.ds(k, 1)] = facing(raw[FIELD, at])[0:1]
        return 0

    lax.fori_loop(0, layers // UNROLL, arrange, 0)

    slots = LANES // 8
    groups = layers // (2 * slots)

    def pack(j, _):
        at = lane // 4
        for a in range(4):
            left, right = zero, zero
            for b in range(2):
                near = zero
                near_slot = part(4 * b - 8 + 8 * gz, 8)
                for i in range(slots):
                    p = 8 * i + 4 * b
                    moved = turn(block[a, 0, j * 2 * slots + b * slots + i], p)
                    right = jnp.where(at == p // 4, moved, right)
                    left = jnp.where(at == (p // 4 - 1) % 32, moved, left)
                    near = jnp.where(near_slot == i, moved, near)
                near_out[a * 2 * groups + 2 * j + b] = near
            far_out[0, a * groups + j] = left
            far_out[1, a * groups + j] = right
        return 0

    lax.fori_loop(0, groups, pack, 0)

    @pl.when(lacks)
    def _():
        for q in range(4):
            for a in range(4):
                for j in range(groups):
                    far_in[q, a * groups + j] = one * 1000.0 if a == LINE else zero

    def factor(q):
        def steps(t, carry):
            carry = list(carry)
            for s in range(UNROLL):
                k = t * UNROLL + s
                line = 1.0 / block[LINE, q, k]
                for h in range(HALF):
                    th, de = carry[2 * h], carry[2 * h + 1]
                    ratio = line * inverses[h]
                    w = ratio * th
                    de = de + w
                    new = th + de
                    theta[h, q, k] = th
                    weight[h, q, k] = w
                    inverse[h, q, k] = 1.0 / (new * th)
                    if q == 0 and h < HALF - 1:
                        theta_out[h, pl.ds(k, 1)] = facing(th)[0:1]
                    carry[2 * h], carry[2 * h + 1] = new, de
            return tuple(carry)

        return lax.fori_loop(0, layers // UNROLL, steps, (one,) * (2 * HALF))

    @pl.when(solver)
    def _():
        def shift_own(t, _):
            for s in range(UNROLL):
                k = t * UNROLL + s
                for a in range(4):
                    block[a, 1, k] = turn(block[a, 0, k], 32)
            return 0

        lax.fori_loop(0, layers // UNROLL, shift_own, 0)

    found = factor(0)
    for h in range(HALF):
        pivots[h, 0] = found[2 * h]
        pivots[h, 1] = found[2 * h + 1]

    pl.semaphore_wait(barrier, 3 + has_left.astype(jnp.int32) + has_right.astype(jnp.int32))

    def send(source, target, send_sem, recv_sem, device):
        return pltpu.make_async_remote_copy(
            src_ref=source,
            dst_ref=target,
            send_sem=send_sem,
            recv_sem=recv_sem,
            device_id=device,
            device_id_type=MESH,
        )

    from_left = 2 * gz + gx
    from_right = 2 * (1 - gz) + gx

    def far(way, quarter):
        device = {"gy": gy + 1 - 2 * way}
        if quarter // 2:
            device["gz"] = 1 - gz
        if quarter % 2 == 0:
            device["gx"] = 1 - gx
        return send(
            far_out.at[way], far_in.at[quarter], far_send.at[way], far_recv.at[quarter], device
        )

    def far_arrival(quarter):
        return send(
            far_out.at[0], far_in.at[quarter], far_send.at[0], far_recv.at[quarter], peers[0]
        )

    def near(x):
        return send(near_out, near_in.at[x], near_send, near_recv.at[x], {"gz": 1 - gz, "gx": 1})

    def near_arrival(x):
        return send(near_out, near_in.at[x], near_send, near_recv.at[x], peers[1])

    def swap(a):
        return send(
            block.at[a, 0], swapped.at[a], swap_send.at[a], swap_recv.at[a], {"gx": 1 - gx}
        )

    def pivot_copy(e):
        return send(pivots, pivots_in.at[e], pivot_send.at[e], pivot_recv.at[e], peers[e])

    def plane_copy(h, e):
        return send(
            planes.at[h], planes_in.at[h, e], plane_send.at[h, e], plane_recv.at[h, e], peers[e]
        )

    def row_copy(h):
        rows = pl.ds(0, layers)
        return send(
            row_out.at[h, rows], row_in.at[h, rows], row_send.at[h], row_recv.at[h], peers[0]
        )

    every = (pl.ds(0, HALF - 1), pl.ds(0, layers))
    theta_copy = send(theta_out.at[every], theta_in.at[every], theta_send, theta_recv, peers[0])

    def strip_copy(e, side):
        return send(
            strip_out, strip_in.at[side], strip_send.at[e], strip_recv.at[side], peers[e]
        )

    def strip_arrival(side):
        return send(
            strip_out, strip_in.at[side], strip_send.at[0], strip_recv.at[side], peers[0]
        )

    row_copy(0).start()
    for way, there, place in ((0, has_right, from_left), (1, has_left, from_right)):
        @pl.when(there)
        def _(way=way, place=place):
            for quarter in range(4):
                @pl.when(place == quarter)
                def _(quarter=quarter):
                    far(way, quarter).start()

    for e in range(3):
        pivot_copy(e).start()
    for x in range(2):
        @pl.when(gx == x)
        def _(x=x):
            near(x).start()

    theta_copy.start()

    @pl.when(gx == 0)
    def _():
        for a in range(4):
            swap(a).start()

    top, bottom = row == 0, row == ROWS - 1
    join = jnp.logical_or(
        jnp.logical_and(top, jnp.logical_not(upper)), jnp.logical_and(bottom, upper)
    )
    keep_up = jnp.where(top, zero, one)
    keep_down = jnp.where(bottom, zero, one)
    keep_left = jnp.where(lane == 0, zero, one)
    keep_right = jnp.where(lane == LANES - 1, zero, one)

    def spread(u, outside):
        up = keep_up * pltpu.roll(u, 1, 0)
        down = keep_down * pltpu.roll(u, ROWS - 1, 0)
        over = jnp.where(join, outside, zero)
        left = keep_left * turn(u, 1)
        right = keep_right * turn(u, -1)
        return ((up + down) + over) + (left + right)

    region = part(-8, 32)
    lower_rows = lax.rem(region, 2) == 1
    cross_up = jnp.logical_and(top, lower_rows)
    cross_down = jnp.logical_and(bottom, jnp.logical_not(lower_rows))

    def strip_spread(u):
        above, below = pltpu.roll(u, 1, 0), pltpu.roll(u, ROWS - 1, 0)
        up = jnp.where(cross_up, turn(above, 32), keep_up * above)
        down = jnp.where(cross_down, turn(below, -32), keep_down * below)
        return (up + down) + (turn(u, 1) + turn(u, -1))

    def eliminate(h, q, values):
        shift = shifts[h]

        def forward(t, total):
            for s in range(SPAN):
                k = t * SPAN + s
                u, beside = values(k)
                flux = block[PLANE, q, k] * (beside - 4.0 * u) + block[SOURCE, q, k]
                total = total + weight[h, q, k] * (u + shift * flux)
                state[q, k] = inverse[h, q, k] * total
            return total

        return lax.fori_loop(0, layers // SPAN, forward, zero)

    def substitute(h, q):
        def backward(t, later):
            for s in range(UNROLL):
                k = layers - 1 - (t * UNROLL + s)
                here = state[q, k]
                if s == 0:
                    here = jnp.where(t == 0, zero, here)
                later = later + here
                state[q, k] = later
                if q == 0 and h < HALF - 1:
                    row_out[h + 1, pl.ds(k, 1)] = facing(later)[0:1]
            return later

        lax.fori_loop(0, layers // UNROLL, backward, zero)

    def targets(h):
        return range(3) if h < HALF - 1 else (1,)

    now = {}

    def run(h):
        end, end_beyond = now.get("end"), now.get("beyond")

        def values(k):
            outside = jnp.broadcast_to(row_in[h, pl.ds(k, 1)], (ROWS, LANES))
            if h == 0:
                u = block[FIELD, 0, k]
            else:
                u = theta[h - 1, 0, k] * (state[0, k] + end)
                outside = jnp.broadcast_to(theta_in[h - 1, pl.ds(k, 1)], (ROWS, LANES)) * (
                    outside + end_beyond
                )
            return u, spread(u, outside)

        total = eliminate(h, 0, values)
        now["total"] = total
        planes[h] = total
        for e in targets(h):
            plane_copy(h, e).start()
        substitute(h, 0)
        if h < HALF - 1:
            row_copy(h + 1).start()

    def settle(h):
        for e in targets(h):
            plane_copy(h, e).wait_recv()
        now["end"] = mixed[0, h, 0] * now["total"] + mixed[0, h, 1] * planes_in[h, 1]
        if h < HALF - 1:
            now["beyond"] = beyond(
                mixed[1, h, 0] * planes_in[h, 0] + mixed[1, h, 1] * planes_in[h, 2]
            )
            row_copy(h + 1).wait_recv()

    def mix(at, h, last, step, other_last, other_step):
        before = last - step
        share = 1.0 / (before * other_step + step * other_last)
        mixed[at, h, 0] = other_last * share / before
        mixed[at, h, 1] = share

    def merge(source, turned, merged, count, quarters):
        for d in range(4):
            for q in range(count):
                for at in range(source.shape[1]):
                    turned[d, q, at] = turn(source[q, at], 32 * d)
        for b in range(2):
            pick = quarters(b)
            for a in range(4):
                for j in range(groups):
                    at = a * groups + j
                    if count == 2:
                        at = a * 2 * groups + 2 * j + b
                    for m in range(4):
                        tiles = [turned[(4 - count + q - m) % 4, q, at] for q in range(count)]
                        tile = tiles[-1]
                        for q in range(count - 1):
                            tile = jnp.where(pick == 4 - count + q, tiles[q], tile)
                        merged[b, (a * groups + j) * 4 + m] = tile

    def strip_near():
        for a in range(4):
            swap(a).wait_recv()
        for x in range(2):
            near_arrival(x).wait_recv()
        merge(near_in, near_turned, near_merged, 2, lambda b: part(4 * b - 8 * gz, 32))

    def strip_far():
        @pl.when(jnp.logical_or(wants_left, wants_right))
        def _():
            for q in range(4):
                far_arrival(q).wait_recv()

        merge(far_in, far_turned, far_merged, 4, lambda b: part(4 * b - 4 + 4 * gz, 32))
        outer = lax.rem(lane + 4 - 4 * gz, 32) < 4

        for n in range(8):
            def gather(j, _, n=n):
                for a in range(4):
                    for m in range(4):
                        at = (a * groups + j) * 4 + m
                        k = j * 2 * slots + 4 * m + n % 2 * slots + n // 2
                        there = turn(near_merged[n % 2, at], -4 * n)
                        tile = turn(far_merged[n % 2, at], -4 * n)
                        own = jnp.where(region == 0, swapped[a, k], block[a, 1, k])
                        own = jnp.where(region < 2, own, there)
                        block[a, 1, k] = jnp.where(outer, tile, own)
                return 0

            lax.fori_loop(0, groups, gather, 0)

        ends = factor(1)
        for h in range(HALF):
            last, step = ends[2 * h], ends[2 * h + 1]
            mix(2, h, last, step, turn(last, half), turn(step, half))

    def strip_run(h):
        end = strip_end[...] if h else None

        def values(k):
            u = theta[h - 1, 1, k] * (state[1, k] + end) if h else block[FIELD, 1, k]
            return u, strip_spread(u)

        total = eliminate(h, 1, values)
        substitute(h, 1)
        strip_end[...] = mixed[2, h, 0] * total + mixed[2, h, 1] * turn(total, half)

    def strip_share():
        end = strip_end[...]
        slot = lax.rem(lane + 4 * gz, 32) // 4

        tiles = [zero] * (layers // 8)
        for i in range(8):
            for v in range(layers // 8):
                k = v * 8 + i
                moved = turn(theta[HALF - 1, 1, k] * (state[1, k] + end), 4 * i)
                tiles[v] = jnp.where(slot == i, moved, tiles[v])
        for v in range(layers // 8):
            strip_out[v] = tiles[v]
        for side in range(2):
            @pl.when(gz == side)
            def _(side=side):
                for e in (1, 2, 0):
                    strip_copy(e, side).start()
                for v in range(layers // 8):
                    strip_in[side, v] = tiles[v]

    row_copy(0).wait_recv()
    run(0)
    for e in range(3):
        pivot_copy(e).wait_recv()
    for h in range(HALF):
        mix(0, h, pivots[h, 0], pivots[h, 1], pivots_in[1, h, 0], pivots_in[1, h, 1])
        if h < HALF - 1:
            mix(1, h, pivots_in[0, h, 0], pivots_in[0, h, 1], pivots_in[2, h, 0], pivots_in[2, h, 1])
    settle(0)
    theta_copy.wait_recv()
    run(1)

    @pl.when(solver)
    def _():
        strip_near()
        strip_far()
        strip_run(0)

    settle(1)
    run(2)

    @pl.when(solver)
    def _():
        strip_run(1)
        strip_run(2)
        strip_run(3)
        strip_share()

    settle(2)
    run(3)

    settle(3)
    end = now["end"]

    @pl.when(jnp.logical_or(gx == 0, gz == 1))
    def _():
        strip_arrival(0).wait_recv()

    @pl.when(jnp.logical_or(gx == 0, gz == 0))
    def _():
        strip_arrival(1).wait_recv()

    lower_core = jnp.full((ROWS, LANES), gx, jnp.int32) == 1
    for side in range(2):
        other_half = jnp.full((ROWS, LANES), gz, jnp.int32) != side
        for v in range(layers // 8):
            tile = strip_in[side, v]
            tile = jnp.where(other_half, turn(tile, half), tile)
            strip_in[side, v] = jnp.where(lower_core, turn(tile, -32), tile)

    for i in range(8):
        for v in range(layers // 8):
            k = v * 8 + i
            left = turn(strip_in[0, v], -4 * i)
            right = turn(strip_in[1, v], -4 * i)
            inner = theta[HALF - 1, 0, k] * (state[0, k] + end)
            inner = jnp.where(lane < 4, left, inner)
            result[layer(k)] = jnp.where(lane >= LANES - 4, right, inner)
    store = pltpu.make_async_copy(result, out_hbm, out_sem)
    store.start()

    for way, there in ((0, has_right), (1, has_left)):
        @pl.when(there)
        def _(way=way):
            far(way, 0).wait_send()

    @pl.when(gx == 0)
    def _():
        for a in range(4):
            swap(a).wait_send()

    @pl.when(solver)
    def _():
        for e in range(3):
            strip_copy(e, 0).wait_send()

    near(0).wait_send()
    theta_copy.wait_send()
    for e in range(3):
        pivot_copy(e).wait_send()
    for h in range(HALF):
        row_copy(h).wait_send()
        for e in targets(h):
            plane_copy(h, e).wait_send()
    store.wait()


def on_device(columns, field, plane, line, source, table, index):
    layers = field.shape[0]
    tile = (ROWS, LANES)
    f32 = jnp.float32
    groups = layers // 32
    dma = pltpu.SemaphoreType.DMA
    return pl.pallas_call(
        functools.partial(kernel, columns),
        out_shape=jax.ShapeDtypeStruct(field.shape, f32),
        in_specs=[pl.BlockSpec(memory_space=pltpu.HBM)] * 6,
        out_specs=pl.BlockSpec(memory_space=pltpu.HBM),
        scratch_shapes=[
            pltpu.SMEM(table.shape, f32),
            pltpu.SMEM(index.shape, jnp.int32),
            pltpu.VMEM((4, layers, *tile), f32),
            pltpu.VMEM((4, 2, layers, *tile), f32),
            pltpu.VMEM((4, layers, *tile), f32),
            pltpu.VMEM((HALF, 2, layers, *tile), f32),
            pltpu.VMEM((HALF, 2, layers, *tile), f32),
            pltpu.VMEM((HALF, 2, layers, *tile), f32),
            pltpu.VMEM((2, layers, *tile), f32),
            pltpu.VMEM((2, 4 * groups, *tile), f32),
            pltpu.VMEM((4, 4 * groups, *tile), f32),
            pltpu.VMEM((8 * groups, *tile), f32),
            pltpu.VMEM((2, 8 * groups, *tile), f32),
            pltpu.VMEM((4, 4, 4 * groups, *tile), f32),
            pltpu.VMEM((4, 2, 8 * groups, *tile), f32),
            pltpu.VMEM((2, 16 * groups, *tile), f32),
            pltpu.VMEM((2, 16 * groups, *tile), f32),
            pltpu.VMEM((layers // 8, *tile), f32),
            pltpu.VMEM((2, layers // 8, *tile), f32),
            pltpu.VMEM(tile, f32),
            pltpu.VMEM((HALF, layers + ROWS, LANES), f32),
            pltpu.VMEM((HALF, layers + ROWS, LANES), f32),
            pltpu.VMEM((HALF - 1, layers + ROWS, LANES), f32),
            pltpu.VMEM((HALF - 1, layers + ROWS, LANES), f32),
            pltpu.VMEM((HALF, 2, *tile), f32),
            pltpu.VMEM((3, HALF, 2, *tile), f32),
            pltpu.VMEM((3, HALF, 2, *tile), f32),
            pltpu.VMEM((HALF, *tile), f32),
            pltpu.VMEM((HALF, 3, *tile), f32),
            pltpu.VMEM((layers, *tile), f32),
            dma((4,)), dma((2,)), dma,
            dma((2,)), dma((4,)), dma, dma((2,)), dma((4,)), dma((4,)), dma((3,)), dma((2,)),
            dma((HALF,)), dma((HALF,)), dma, dma, dma((3,)), dma((3,)), dma((HALF, 3)), dma((HALF, 3)),
        ],
        compiler_params=pltpu.CompilerParams(
            collective_id=0, has_side_effects=True, vmem_limit_bytes=67043328
        ),
    )(field, plane, line, source, table, index)


def solution(mesh):
    spec = P("gz", "gx", "gy")
    return jax.shard_map(
        functools.partial(on_device, mesh.shape["gy"]),
        mesh=mesh,
        in_specs=(spec, spec, spec, spec, P(), P()),
        out_specs=spec,
        check_vma=False,
    )
```

```python
import functools
import jax
import jax.numpy as jnp
from jax import lax
from jax.experimental import pallas as pl
from jax.experimental.pallas import tpu as pltpu
from jax.sharding import PartitionSpec as P

HALF = 4
ROWS = 8
LANES = 128
UNROLL = 16
SPAN = 64
FIELD, PLANE, LINE, SOURCE = range(4)
MESH = pl.DeviceIdType.MESH


def turn(tile, shift):
    shift %= LANES
    return pltpu.roll(tile, shift, 1) if shift else tile


def kernel(
    columns,
    field_hbm, plane_hbm, line_hbm, source_hbm, table_hbm, index_hbm,
    out_hbm,
    table, index, raw, block, swapped, theta, weight, inverse, state,
    far_out, far_in, near_out, near_in, far_turned, near_turned, far_merged, near_merged, strip_out, strip_in, strip_end,
    row_out, row_in, theta_out, theta_in,
    pivots, pivots_in, mixed, planes, planes_in, result,
    local_sem, scalar_sem, out_sem,
    far_send, far_recv, near_send, near_recv, swap_send, swap_recv, strip_send, strip_recv,
    row_send, row_recv, theta_send, theta_recv, pivot_send, pivot_recv, plane_send, plane_recv,
):
    layers = field_hbm.shape[0]
    gz, gx, gy = lax.axis_index("gz"), lax.axis_index("gx"), lax.axis_index("gy")
    has_left, has_right = gy > 0, gy < columns - 1
    solver = gx == 1
    wants_left = jnp.logical_and(solver, jnp.logical_and(gz == 0, has_left))
    wants_right = jnp.logical_and(solver, jnp.logical_and(gz == 1, has_right))
    lacks = jnp.logical_and(
        solver, jnp.logical_not(jnp.logical_or(wants_left, wants_right))
    )
    lane = lax.broadcasted_iota(jnp.int32, (ROWS, LANES), 1)
    row = lax.broadcasted_iota(jnp.int32, (ROWS, LANES), 0)
    zero = jnp.zeros((ROWS, LANES), jnp.float32)
    one = jnp.ones((ROWS, LANES), jnp.float32)
    upper = jnp.full((ROWS, LANES), gx, jnp.int32) == 0
    half = LANES // 2

    def part(offset, size):
        return lax.rem(lane - offset + LANES, LANES) // size

    def layer(k):
        return gz * (layers - 1) + (1 - 2 * gz) * k

    peers = (
        {"gx": 1 - gx},
        {"gz": 1 - gz},
        {"gz": 1 - gz, "gx": 1 - gx},
    )

    def facing(tile):
        return jnp.where(upper, pltpu.roll(tile, 1, 0), tile)

    def beyond(tile):
        first = jnp.broadcast_to(tile[0:1], (ROWS, LANES))
        last = jnp.broadcast_to(tile[ROWS - 1 : ROWS], (ROWS, LANES))
        return jnp.where(upper, first, last)

    loads = [
        pltpu.make_async_copy(source, raw.at[a], local_sem.at[a])
        for a, source in enumerate((field_hbm, plane_hbm, line_hbm, source_hbm))
    ]
    scalars = [
        pltpu.make_async_copy(table_hbm, table, scalar_sem.at[0]),
        pltpu.make_async_copy(index_hbm, index, scalar_sem.at[1]),
    ]
    for copy in scalars + loads:
        copy.start()

    barrier = pltpu.get_barrier_semaphore()
    beside = ({}, {"gx": 1 - gx}, {"gz": 1 - gz}, {"gz": 1 - gz, "gx": 1 - gx})
    for step, wanted in ((-1, wants_left), (1, wants_right)):
        @pl.when(wanted)
        def _(step=step):
            for other in beside:
                pl.semaphore_signal(
                    barrier, inc=1, device_id={"gy": gy + step, **other}, device_id_type=MESH
                )

    for peer in peers:
        pl.semaphore_signal(barrier, inc=1, device_id=peer, device_id_type=MESH)

    for copy in scalars:
        copy.wait()
    shifts = [jnp.full((ROWS, LANES), table[index[h]], jnp.float32) for h in range(HALF)]
    inverses = [1.0 / s for s in shifts]

    for copy in loads:
        copy.wait()

    def arrange(t, _):
        for s in range(UNROLL):
            k = t * UNROLL + s
            at = layer(k)
            for a in range(4):
                block[a, 0, k] = raw[a, at]
            row_out[0, pl.ds(k, 1)] = facing(raw[FIELD, at])[0:1]
        return 0

    lax.fori_loop(0, layers // UNROLL, arrange, 0)

    slots = LANES // 8
    groups = layers // (2 * slots)

    near_slots = [part(4 * b - 8 + 8 * gz, 8) for b in range(2)]
    quad = lane // 4

    def pack(a, _):
        left, right = [zero] * groups, [zero] * groups
        near = [zero] * (2 * groups)
        for n in range(2 * slots):
            i, b = n // 2, n % 2
            for j in range(groups):
                moved = turn(block[a, 0, j * 2 * slots + b * slots + i], 4 * n)
                right[j] = jnp.where(quad == n, moved, right[j])
                left[j] = jnp.where(quad == (n - 1) % 32, moved, left[j])
                near[2 * j + b] = jnp.where(near_slots[b] == i, moved, near[2 * j + b])
        for j in range(groups):
            far_out[0, a * groups + j] = left[j]
            far_out[1, a * groups + j] = right[j]
        for j in range(2 * groups):
            near_out[a * 2 * groups + j] = near[j]
        return 0

    lax.fori_loop(0, 4, pack, 0)

    @pl.when(lacks)
    def _():
        for q in range(4):
            for a in range(4):
                for j in range(groups):
                    far_in[q, a * groups + j] = one * 1000.0 if a == LINE else zero

    def factor(q):
        def steps(t, carry):
            carry = list(carry)
            for s in range(UNROLL):
                k = t * UNROLL + s
                line = 1.0 / block[LINE, q, k]
                for h in range(HALF):
                    th, de = carry[2 * h], carry[2 * h + 1]
                    ratio = line * inverses[h]
                    w = ratio * th
                    de = de + w
                    new = th + de
                    theta[h, q, k] = th
                    weight[h, q, k] = w
                    inverse[h, q, k] = 1.0 / (new * th)
                    if q == 0 and h < HALF - 1:
                        theta_out[h, pl.ds(k, 1)] = facing(th)[0:1]
                    carry[2 * h], carry[2 * h + 1] = new, de
            return tuple(carry)

        return lax.fori_loop(0, layers // UNROLL, steps, (one,) * (2 * HALF))

    @pl.when(solver)
    def _():
        def shift_own(t, _):
            for s in range(UNROLL):
                k = t * UNROLL + s
                for a in range(4):
                    block[a, 1, k] = turn(block[a, 0, k], 32)
            return 0

        lax.fori_loop(0, layers // UNROLL, shift_own, 0)

    found = factor(0)
    for h in range(HALF):
        pivots[h, 0] = found[2 * h]
        pivots[h, 1] = found[2 * h + 1]

    pl.semaphore_wait(barrier, 3 + has_left.astype(jnp.int32) + has_right.astype(jnp.int32))

    def send(source, target, send_sem, recv_sem, device):
        return pltpu.make_async_remote_copy(
            src_ref=source,
            dst_ref=target,
            send_sem=send_sem,
            recv_sem=recv_sem,
            device_id=device,
            device_id_type=MESH,
        )

    from_left = 2 * gz + gx
    from_right = 2 * (1 - gz) + gx

    def far(way, quarter):
        device = {"gy": gy + 1 - 2 * way}
        if quarter // 2:
            device["gz"] = 1 - gz
        if quarter % 2 == 0:
            device["gx"] = 1 - gx
        return send(
            far_out.at[way], far_in.at[quarter], far_send.at[way], far_recv.at[quarter], device
        )

    def far_arrival(quarter):
        return send(
            far_out.at[0], far_in.at[quarter], far_send.at[0], far_recv.at[quarter], peers[0]
        )

    def near(x):
        return send(near_out, near_in.at[x], near_send, near_recv.at[x], {"gz": 1 - gz, "gx": 1})

    def near_arrival(x):
        return send(near_out, near_in.at[x], near_send, near_recv.at[x], peers[1])

    def swap(a):
        return send(
            block.at[a, 0], swapped.at[a], swap_send.at[a], swap_recv.at[a], {"gx": 1 - gx}
        )

    def pivot_copy(e):
        return send(pivots, pivots_in.at[e], pivot_send.at[e], pivot_recv.at[e], peers[e])

    def plane_copy(h, e):
        return send(
            planes.at[h], planes_in.at[h, e], plane_send.at[h, e], plane_recv.at[h, e], peers[e]
        )

    def row_copy(h):
        rows = pl.ds(0, layers)
        return send(
            row_out.at[h, rows], row_in.at[h, rows], row_send.at[h], row_recv.at[h], peers[0]
        )

    every = (pl.ds(0, HALF - 1), pl.ds(0, layers))
    theta_copy = send(theta_out.at[every], theta_in.at[every], theta_send, theta_recv, peers[0])

    def strip_copy(e, side):
        return send(
            strip_out, strip_in.at[side], strip_send.at[e], strip_recv.at[side], peers[e]
        )

    def strip_arrival(side):
        return send(
            strip_out, strip_in.at[side], strip_send.at[0], strip_recv.at[side], peers[0]
        )

    row_copy(0).start()
    for way, there, place in ((0, has_right, from_left), (1, has_left, from_right)):
        @pl.when(there)
        def _(way=way, place=place):
            for quarter in range(4):
                @pl.when(place == quarter)
                def _(quarter=quarter):
                    far(way, quarter).start()

    for e in range(3):
        pivot_copy(e).start()
    for x in range(2):
        @pl.when(gx == x)
        def _(x=x):
            near(x).start()

    theta_copy.start()

    @pl.when(gx == 0)
    def _():
        for a in range(4):
            swap(a).start()

    top, bottom = row == 0, row == ROWS - 1
    join = jnp.logical_or(
        jnp.logical_and(top, jnp.logical_not(upper)), jnp.logical_and(bottom, upper)
    )
    keep_up = jnp.where(top, zero, one)
    keep_down = jnp.where(bottom, zero, one)
    keep_left = jnp.where(lane == 0, zero, one)
    keep_right = jnp.where(lane == LANES - 1, zero, one)

    def spread(u, outside):
        up = keep_up * pltpu.roll(u, 1, 0)
        down = keep_down * pltpu.roll(u, ROWS - 1, 0)
        over = jnp.where(join, outside, zero)
        left = keep_left * turn(u, 1)
        right = keep_right * turn(u, -1)
        return ((up + down) + over) + (left + right)

    region = part(-8, 32)
    lower_rows = lax.rem(region, 2) == 1
    cross_up = jnp.logical_and(top, lower_rows)
    cross_down = jnp.logical_and(bottom, jnp.logical_not(lower_rows))

    def strip_spread(u):
        above, below = pltpu.roll(u, 1, 0), pltpu.roll(u, ROWS - 1, 0)
        up = jnp.where(cross_up, turn(above, 32), keep_up * above)
        down = jnp.where(cross_down, turn(below, -32), keep_down * below)
        return (up + down) + (turn(u, 1) + turn(u, -1))

    def eliminate(h, q, values):
        shift = shifts[h]

        def forward(t, total):
            for s in range(SPAN):
                k = t * SPAN + s
                u, beside = values(k)
                flux = block[PLANE, q, k] * (beside - 4.0 * u) + block[SOURCE, q, k]
                total = total + weight[h, q, k] * (u + shift * flux)
                state[q, k] = inverse[h, q, k] * total
            return total

        return lax.fori_loop(0, layers // SPAN, forward, zero)

    def substitute(h, q):
        def backward(t, later):
            for s in range(UNROLL):
                k = layers - 1 - (t * UNROLL + s)
                here = state[q, k]
                if s == 0:
                    here = jnp.where(t == 0, zero, here)
                later = later + here
                state[q, k] = later
                if q == 0 and h < HALF - 1:
                    row_out[h + 1, pl.ds(k, 1)] = facing(later)[0:1]
            return later

        lax.fori_loop(0, layers // UNROLL, backward, zero)

    def targets(h):
        return range(3) if h < HALF - 1 else (1,)

    now = {}

    def run(h):
        end, end_beyond = now.get("end"), now.get("beyond")

        def values(k):
            outside = jnp.broadcast_to(row_in[h, pl.ds(k, 1)], (ROWS, LANES))
            if h == 0:
                u = block[FIELD, 0, k]
            else:
                u = theta[h - 1, 0, k] * (state[0, k] + end)
                outside = jnp.broadcast_to(theta_in[h - 1, pl.ds(k, 1)], (ROWS, LANES)) * (
                    outside + end_beyond
                )
            return u, spread(u, outside)

        total = eliminate(h, 0, values)
        now["total"] = total
        planes[h] = total
        for e in targets(h):
            plane_copy(h, e).start()
        substitute(h, 0)
        if h < HALF - 1:
            row_copy(h + 1).start()

    def settle(h):
        for e in targets(h):
            plane_copy(h, e).wait_recv()
        now["end"] = mixed[0, h, 0] * now["total"] + mixed[0, h, 1] * planes_in[h, 1]
        if h < HALF - 1:
            now["beyond"] = beyond(
                mixed[1, h, 0] * planes_in[h, 0] + mixed[1, h, 1] * planes_in[h, 2]
            )
            row_copy(h + 1).wait_recv()

    def mix(at, h, last, step, other_last, other_step):
        before = last - step
        share = 1.0 / (before * other_step + step * other_last)
        mixed[at, h, 0] = other_last * share / before
        mixed[at, h, 1] = share

    def merge(source, turned, merged, count, quarters):
        for d in range(4):
            for q in range(count):
                for at in range(source.shape[1]):
                    turned[d, q, at] = turn(source[q, at], 32 * d)
        for b in range(2):
            pick = quarters(b)
            for a in range(4):
                for j in range(groups):
                    at = a * groups + j
                    if count == 2:
                        at = a * 2 * groups + 2 * j + b
                    for m in range(4):
                        tiles = [turned[(4 - count + q - m) % 4, q, at] for q in range(count)]
                        tile = tiles[-1]
                        for q in range(count - 1):
                            tile = jnp.where(pick == 4 - count + q, tiles[q], tile)
                        merged[b, (a * groups + j) * 4 + m] = tile

    def strip_near():
        for a in range(4):
            swap(a).wait_recv()
        for x in range(2):
            near_arrival(x).wait_recv()
        merge(near_in, near_turned, near_merged, 2, lambda b: part(4 * b - 8 * gz, 32))

    def strip_far():
        @pl.when(jnp.logical_or(wants_left, wants_right))
        def _():
            for q in range(4):
                far_arrival(q).wait_recv()

        merge(far_in, far_turned, far_merged, 4, lambda b: part(4 * b - 4 + 4 * gz, 32))
        outer = lax.rem(lane + 4 - 4 * gz, 32) < 4

        for n in range(8):
            def gather(j, _, n=n):
                for a in range(4):
                    for m in range(4):
                        at = (a * groups + j) * 4 + m
                        k = j * 2 * slots + 4 * m + n % 2 * slots + n // 2
                        there = turn(near_merged[n % 2, at], -4 * n)
                        tile = turn(far_merged[n % 2, at], -4 * n)
                        own = jnp.where(region == 0, swapped[a, k], block[a, 1, k])
                        own = jnp.where(region < 2, own, there)
                        block[a, 1, k] = jnp.where(outer, tile, own)
                return 0

            lax.fori_loop(0, groups, gather, 0)

        ends = factor(1)
        for h in range(HALF):
            last, step = ends[2 * h], ends[2 * h + 1]
            mix(2, h, last, step, turn(last, half), turn(step, half))

    def strip_run(h):
        end = strip_end[...] if h else None

        def values(k):
            u = theta[h - 1, 1, k] * (state[1, k] + end) if h else block[FIELD, 1, k]
            return u, strip_spread(u)

        total = eliminate(h, 1, values)
        substitute(h, 1)
        strip_end[...] = mixed[2, h, 0] * total + mixed[2, h, 1] * turn(total, half)

    def strip_share():
        end = strip_end[...]
        slot = lax.rem(lane + 4 * gz, 32) // 4

        tiles = [zero] * (layers // 8)
        for i in range(8):
            for v in range(layers // 8):
                k = v * 8 + i
                moved = turn(theta[HALF - 1, 1, k] * (state[1, k] + end), 4 * i)
                tiles[v] = jnp.where(slot == i, moved, tiles[v])
        for v in range(layers // 8):
            strip_out[v] = tiles[v]
        for side in range(2):
            @pl.when(gz == side)
            def _(side=side):
                for e in (1, 2, 0):
                    strip_copy(e, side).start()
                for v in range(layers // 8):
                    strip_in[side, v] = tiles[v]

    row_copy(0).wait_recv()
    run(0)
    for e in range(3):
        pivot_copy(e).wait_recv()
    for h in range(HALF):
        mix(0, h, pivots[h, 0], pivots[h, 1], pivots_in[1, h, 0], pivots_in[1, h, 1])
        if h < HALF - 1:
            mix(1, h, pivots_in[0, h, 0], pivots_in[0, h, 1], pivots_in[2, h, 0], pivots_in[2, h, 1])
    settle(0)
    theta_copy.wait_recv()
    run(1)

    @pl.when(solver)
    def _():
        strip_near()
        strip_far()
        strip_run(0)

    settle(1)
    run(2)

    @pl.when(solver)
    def _():
        strip_run(1)
        strip_run(2)
        strip_run(3)
        strip_share()

    settle(2)
    run(3)

    settle(3)
    end = now["end"]

    @pl.when(jnp.logical_or(gx == 0, gz == 1))
    def _():
        strip_arrival(0).wait_recv()

    @pl.when(jnp.logical_or(gx == 0, gz == 0))
    def _():
        strip_arrival(1).wait_recv()

    lower_core = jnp.full((ROWS, LANES), gx, jnp.int32) == 1
    for side in range(2):
        other_half = jnp.full((ROWS, LANES), gz, jnp.int32) != side
        for v in range(layers // 8):
            tile = strip_in[side, v]
            tile = jnp.where(other_half, turn(tile, half), tile)
            strip_in[side, v] = jnp.where(lower_core, turn(tile, -32), tile)

    for i in range(8):
        for v in range(layers // 8):
            k = v * 8 + i
            left = turn(strip_in[0, v], -4 * i)
            right = turn(strip_in[1, v], -4 * i)
            inner = theta[HALF - 1, 0, k] * (state[0, k] + end)
            inner = jnp.where(lane < 4, left, inner)
            result[layer(k)] = jnp.where(lane >= LANES - 4, right, inner)
    store = pltpu.make_async_copy(result, out_hbm, out_sem)
    store.start()

    for way, there in ((0, has_right), (1, has_left)):
        @pl.when(there)
        def _(way=way):
            far(way, 0).wait_send()

    @pl.when(gx == 0)
    def _():
        for a in range(4):
            swap(a).wait_send()

    @pl.when(solver)
    def _():
        for e in range(3):
            strip_copy(e, 0).wait_send()

    near(0).wait_send()
    theta_copy.wait_send()
    for e in range(3):
        pivot_copy(e).wait_send()
    for h in range(HALF):
        row_copy(h).wait_send()
        for e in targets(h):
            plane_copy(h, e).wait_send()
    store.wait()


def on_device(columns, field, plane, line, source, table, index):
    layers = field.shape[0]
    tile = (ROWS, LANES)
    f32 = jnp.float32
    groups = layers // 32
    dma = pltpu.SemaphoreType.DMA
    return pl.pallas_call(
        functools.partial(kernel, columns),
        out_shape=jax.ShapeDtypeStruct(field.shape, f32),
        in_specs=[pl.BlockSpec(memory_space=pltpu.HBM)] * 6,
        out_specs=pl.BlockSpec(memory_space=pltpu.HBM),
        scratch_shapes=[
            pltpu.SMEM(table.shape, f32),
            pltpu.SMEM(index.shape, jnp.int32),
            pltpu.VMEM((4, layers, *tile), f32),
            pltpu.VMEM((4, 2, layers, *tile), f32),
            pltpu.VMEM((4, layers, *tile), f32),
            pltpu.VMEM((HALF, 2, layers, *tile), f32),
            pltpu.VMEM((HALF, 2, layers, *tile), f32),
            pltpu.VMEM((HALF, 2, layers, *tile), f32),
            pltpu.VMEM((2, layers, *tile), f32),
            pltpu.VMEM((2, 4 * groups, *tile), f32),
            pltpu.VMEM((4, 4 * groups, *tile), f32),
            pltpu.VMEM((8 * groups, *tile), f32),
            pltpu.VMEM((2, 8 * groups, *tile), f32),
            pltpu.VMEM((4, 4, 4 * groups, *tile), f32),
            pltpu.VMEM((4, 2, 8 * groups, *tile), f32),
            pltpu.VMEM((2, 16 * groups, *tile), f32),
            pltpu.VMEM((2, 16 * groups, *tile), f32),
            pltpu.VMEM((layers // 8, *tile), f32),
            pltpu.VMEM((2, layers // 8, *tile), f32),
            pltpu.VMEM(tile, f32),
            pltpu.VMEM((HALF, layers + ROWS, LANES), f32),
            pltpu.VMEM((HALF, layers + ROWS, LANES), f32),
            pltpu.VMEM((HALF - 1, layers + ROWS, LANES), f32),
            pltpu.VMEM((HALF - 1, layers + ROWS, LANES), f32),
            pltpu.VMEM((HALF, 2, *tile), f32),
            pltpu.VMEM((3, HALF, 2, *tile), f32),
            pltpu.VMEM((3, HALF, 2, *tile), f32),
            pltpu.VMEM((HALF, *tile), f32),
            pltpu.VMEM((HALF, 3, *tile), f32),
            pltpu.VMEM((layers, *tile), f32),
            dma((4,)), dma((2,)), dma,
            dma((2,)), dma((4,)), dma, dma((2,)), dma((4,)), dma((4,)), dma((3,)), dma((2,)),
            dma((HALF,)), dma((HALF,)), dma, dma, dma((3,)), dma((3,)), dma((HALF, 3)), dma((HALF, 3)),
        ],
        compiler_params=pltpu.CompilerParams(
            collective_id=0, has_side_effects=True, vmem_limit_bytes=67043328
        ),
    )(field, plane, line, source, table, index)


def solution(mesh):
    spec = P("gz", "gx", "gy")
    return jax.shard_map(
        functools.partial(on_device, mesh.shape["gy"]),
        mesh=mesh,
        in_specs=(spec, spec, spec, spec, P(), P()),
        out_specs=spec,
        check_vma=False,
    )
```
